32 devices in a mesh: dp: 8 (over y, x, core), tensor: 4 (over z).
Axes of the slice: x: 2, y: 2, z: 4, core: 2. Of those that a mesh axis runs over, the one named last changes fastest.
Arguments:
- tokens: bfloat16 [16384, 768], P(('dp', 'tensor')), may hold values from -6 to 6
- segments: int32 [16384], P('dp'), may hold values from -1 to 9, as said below
- cotangent: bfloat16 [16384, 768], P(('dp', 'tensor')), may hold values from -6 to 6
- ln1_gain: bfloat16 [768], replicated, may hold values from 0.5 to 1.5
- ln1_bias: bfloat16 [768], replicated, may hold values from -2 to 2
- w_qkv: bfloat16 [768, 2304], P(None, 'tensor'), may hold values from -0.21875 to 0.21875
- q_bias: bfloat16 [768], P('tensor'), may hold values from -3 to 3
- v_bias: bfloat16 [768], P('tensor'), may hold values from -3 to 3
- w_out: bfloat16 [768, 768], P('tensor'), may hold values from -0.625 to 0.625
- out_bias: bfloat16 [768], replicated, may hold values from -2 to 2
- ln2_gain: bfloat16 [768], replicated, may hold values from 0.5 to 1.5
- ln2_bias: bfloat16 [768], replicated, may hold values from -2 to 2
- w_fc1: bfloat16 [768, 3072], P(None, 'tensor'), may hold values from -0.21875 to 0.21875
- fc1_bias: bfloat16 [3072], P('tensor'), may hold values from -3 to 3
- w_fc2: bfloat16 [3072, 768], P('tensor'), may hold values from -0.109375 to 0.109375
- fc2_bias: bfloat16 [768], replicated, may hold values from -2 to 2
Outputs:
- output: bfloat16 [16384, 768], P(('dp', 'tensor'))
- grad_tokens: bfloat16 [16384, 768], P(('dp', 'tensor'))
- cls_features: float32 [16384, 768], P(('dp', 'tensor'))
- grad_w_qkv: float32 [768, 2304], P('dp', 'tensor')
- grad_q_bias: float32 [768], replicated
- grad_v_bias: float32 [768], replicated
- grad_w_out: float32 [768, 768], P('tensor', 'dp')
- grad_out_bias: float32 [768], replicated
- grad_w_fc1: float32 [768, 3072], P('dp', 'tensor')
- grad_fc1_bias: float32 [3072], replicated
- grad_w_fc2: float32 [3072, 768], P('tensor', 'dp')
- grad_fc2_bias: float32 [768], replicated
- grad_ln1_gain: float32 [768], replicated
- grad_ln1_bias: float32 [768], replicated
- grad_ln2_gain: float32 [768], replicated
- grad_ln2_bias: float32 [768], replicated
The draws below stay inside these ranges and needn't reach their ends.
Inputs may be any that keep to these rules, and one draw needn't show every extreme that they name: `segments`: within each aligned block of 512 positions the ids run 0, 1, 2, ... in order, id i over a run of 1 + 49 v positions with v from 1 to 4, starting at the block's first position; positions after the block's last whole sample hold -1. The first block begins with a run of 197; the last block holds only runs of 50, as many as fit.
All inputs are finite; a program needn't handle non-finite values.
Results may differ from the reference program's by a relative error of at most 0.024.
Values may be sent and summed in bfloat16 or wider, within the bound.
A program may use at most 128 MiB of HBM per device.

```python
import math
import jax
import jax.numpy as jnp
from jax import lax

D = 768
H = 12
HD = 64
FF = 3072
SEQ = 512
PATCHES = 49
VIEWS = 4
TOKENS = 16384


def draw_segments(key, part):
    blocks = TOKENS // SEQ
    slots = SEQ // (PATCHES + 1) + 1
    views = jax.random.randint(key, (blocks, slots), 1, VIEWS + 1)
    views = views.at[blocks - 1].set(1)
    views = views.at[0, 0].set(VIEWS)
    lengths = 1 + PATCHES * views
    ends = jnp.cumsum(lengths, axis=1)
    fitted = jnp.max(jnp.where(ends <= SEQ, ends, 0), axis=1)
    positions = jnp.arange(SEQ)
    index = jnp.sum((ends[:, None, :] <= positions[None, :, None]).astype(jnp.int32), axis=-1)
    labels = jnp.where(positions[None, :] < fitted[:, None], index, -1)
    return labels.reshape(-1).astype(jnp.int32)


def shard_levels(key, extent, pieces, least, high):
    loudness, own = 1.0, jax.random.fold_in(key, 6)
    for dim, blocks in pieces:
        steps = jnp.exp(jax.random.uniform(jax.random.fold_in(own, dim), (blocks,), jnp.float32, least / len(pieces), high / len(pieces)))
        loudness = loudness * jnp.repeat(steps, extent[dim] // blocks).reshape([-1 if axis == dim else 1 for axis in range(len(extent))])
    return loudness


def noise(key, extent, deviation, limit, split=(), held_as=jnp.bfloat16):
    entries = deviation * jax.random.normal(key, extent, jnp.float32)
    if split:
        entries = entries * shard_levels(key, extent, split, -0.22, 0.18)
    return jnp.clip(entries, -limit, limit).astype(held_as)


def setup_inputs(seed: int = 0) -> dict:
    keys = jax.random.split(jax.random.key(seed), 17)
    tokens = noise(keys[0], (TOKENS, D), 1.0, 6.0, ((0, 32),))
    segments = draw_segments(jax.random.fold_in(keys[16], 71), 0)
    cotangent = noise(keys[2], (TOKENS, D), 1.0, 6.0, ((0, 32),))
    ln1_gain = jnp.clip(1.0 + 0.1 * jax.random.normal(keys[3], (D,), jnp.float32), 0.5, 1.5).astype(jnp.bfloat16)
    ln1_bias = noise(keys[4], (D,), 0.3, 2.0)
    w_qkv = noise(keys[5], (D, H * 3 * HD), D ** -0.5, 0.21875, ((1, 4),))
    q_bias = noise(keys[6], (H * HD,), 0.5, 3.0, ((0, 4),))
    v_bias = noise(keys[7], (H * HD,), 0.5, 3.0, ((0, 4),))
    w_out = noise(keys[8], (H * HD, D), (H * HD // 8) ** -0.5, 0.625, ((0, 4),))
    out_bias = noise(keys[9], (D,), 0.3, 2.0)
    ln2_gain = jnp.clip(1.0 + 0.1 * jax.random.normal(keys[10], (D,), jnp.float32), 0.5, 1.5).astype(jnp.bfloat16)
    ln2_bias = noise(keys[11], (D,), 0.3, 2.0)
    w_fc1 = noise(keys[12], (D, FF), D ** -0.5, 0.21875, ((1, 4),))
    fc1_bias = noise(keys[13], (FF,), 0.5, 3.0, ((0, 4),))
    w_fc2 = noise(keys[14], (FF, D), FF ** -0.5, 0.109375, ((0, 4),))
    fc2_bias = noise(keys[15], (D,), 0.3, 2.0)
    return dict(tokens=tokens, segments=segments, cotangent=cotangent, ln1_gain=ln1_gain, ln1_bias=ln1_bias, w_qkv=w_qkv, q_bias=q_bias, v_bias=v_bias, w_out=w_out, out_bias=out_bias, ln2_gain=ln2_gain, ln2_bias=ln2_bias, w_fc1=w_fc1, fc1_bias=fc1_bias, w_fc2=w_fc2, fc2_bias=fc2_bias)


@jax.custom_vjp
def low(v):
    return lax.optimization_barrier(v.astype(jnp.bfloat16)).astype(jnp.float32)

@jax.custom_vjp
def low_back(v):
    return v

def low_keep(v):
    return (low(v), None)

def low_pass(kept, grad):
    return (grad,)

def back_keep(v):
    return (v, None)

def back_low(kept, grad):
    return (low(grad),)
low.defvjp(low_keep, low_pass)
low_back.defvjp(back_keep, back_low)

def exact_dot(left, right):
    return jnp.dot(left, right, precision=lax.Precision.HIGHEST, preferred_element_type=jnp.float32)

def layer_norm(values, gain, shift):
    average = lax.optimization_barrier(jnp.mean(values, axis=-1, keepdims=True))
    centered = values - average
    spread = lax.optimization_barrier(jnp.mean(centered * centered, axis=-1, keepdims=True))
    return centered * lax.rsqrt(spread + 1e-06) * gain + shift

def first_flags(segments):
    positions = jnp.arange(segments.shape[0]) % SEQ
    earlier = jnp.concatenate([jnp.full((1,), -2, jnp.int32), segments[:-1].astype(jnp.int32)])
    return ((segments >= 0) & ((positions == 0) | (segments != earlier))).astype(jnp.float32)

def attend_block(inputs):
    queries, key_rows, value_rows, labels = inputs
    scores = jnp.einsum('qhd,khd->hqk', queries, key_rows, precision=lax.Precision.HIGHEST) * (1.0 / math.sqrt(HD))
    scores = low_back(scores)
    same_sample = labels[:, None] == labels[None, :]
    scores = jnp.where(same_sample[None], scores, -1e+30)
    highest = lax.optimization_barrier(jnp.max(scores, axis=-1, keepdims=True))
    expon = jnp.exp(scores - highest)
    weights = low(expon / lax.optimization_barrier(jnp.sum(expon, axis=-1, keepdims=True)))
    return jnp.einsum('hqk,khd->qhd', weights, value_rows, precision=lax.Precision.HIGHEST)

def reference(tokens, segments, cotangent, ln1_gain, ln1_bias, w_qkv, q_bias, v_bias, w_out, out_bias, ln2_gain, ln2_bias, w_fc1, fc1_bias, w_fc2, fc2_bias):
    floats = [array.astype(jnp.float32) for array in (tokens, ln1_gain, ln1_bias, w_qkv, q_bias, v_bias, w_out, out_bias, ln2_gain, ln2_bias, w_fc1, fc1_bias, w_fc2, fc2_bias)]
    labels = segments.reshape(-1, SEQ)

    def forward(inputs, gain_one, shift_one, weight_qkv, bias_query, bias_value, weight_out, bias_out, gain_two, shift_two, weight_one, bias_one, weight_two, bias_two):
        total = inputs.shape[0]
        normed = low(layer_norm(inputs, gain_one, shift_one))
        mixed = exact_dot(normed, weight_qkv).reshape(total, H, 3, HD)
        queries = low_back(low(mixed[:, :, 0] + bias_query.reshape(H, HD)))
        key_rows = low_back(low(mixed[:, :, 1]))
        value_rows = low_back(low(mixed[:, :, 2] + bias_value.reshape(H, HD)))
        blocked = lambda array: array.reshape(-1, SEQ, H, HD)
        attended = lax.map(jax.checkpoint(attend_block), (blocked(queries), blocked(key_rows), blocked(value_rows), labels))
        heads = low_back(low(attended.reshape(total, H * HD)))
        resid = inputs + low_back(exact_dot(heads, weight_out)) + bias_out
        normed_two = low(layer_norm(resid, gain_two, shift_two))
        hidden = low_back(exact_dot(normed_two, weight_one) + bias_one)
        active = low(jax.nn.gelu(hidden, approximate=False))
        return resid + low_back(exact_dot(active, weight_two)) + bias_two
    output, backward = jax.vjp(forward, *floats)
    live = (segments >= 0).astype(jnp.float32)
    grads = backward(cotangent.astype(jnp.float32) * live[:, None])
    out_low = output.astype(jnp.bfloat16)
    flags = first_flags(segments)[:, None]
    values = out_low.astype(jnp.float32)
    cls_count = jnp.sum(flags)
    average = lax.optimization_barrier(jnp.sum(flags * values, axis=0)) / cls_count
    spread = lax.optimization_barrier(jnp.sum(flags * values * values, axis=0)) / cls_count - average * average
    cls_features = flags * (values - average) * lax.rsqrt(spread + 1e-05)
    return (out_low, grads[0].astype(jnp.bfloat16), cls_features, grads[3], grads[4], grads[5], grads[6], grads[7], grads[10], grads[11], grads[12], grads[13], grads[1], grads[2], grads[8], grads[9])
```

```python
from functools import partial
import math

import jax
import jax.numpy as jnp
from jax import lax
from jax.experimental import pallas as pl
from jax.experimental.pallas import tpu as pltpu
from jax.sharding import PartitionSpec as P

HD = 64
SEQ = 512
FAN = 8
F32 = jnp.float32
BF16 = jnp.bfloat16
MESH = pl.DeviceIdType.MESH
ANY = pl.BlockSpec(memory_space=pl.ANY)
VMEM = pl.BlockSpec(memory_space=pltpu.VMEM)


class Place:
    def __init__(self, dp_size, parts):
        self.d = lax.axis_index("dp")
        self.t = lax.axis_index("tensor")
        self.dp_size, self.parts = dp_size, parts
        self.low = dp_size // FAN
        block = self.d // self.low
        self.y, self.x, self.c = block // 4, (block // 2) % 2, block % 2

    def flip(self, name):
        stride = self.low * {"y": 4, "x": 2, "c": 1}[name]
        bit = {"y": self.y, "x": self.x, "c": self.c}[name]
        return (self.d + stride * (1 - 2 * bit), self.t)

    def flip_stride(self, stride):
        bit = (self.d // stride) % 2
        return (self.d + stride * (1 - 2 * bit), self.t)

    def shift(self, k):
        return (self.d, (self.t + k) % self.parts)


def greet(partners):
    barrier = pltpu.get_barrier_semaphore()
    for partner in partners:
        pl.semaphore_signal(barrier, inc=1, device_id=partner, device_id_type=MESH)
    pl.semaphore_wait(barrier, len(partners))


class Link:
    def __init__(self, send_sem, recv_sem):
        self.send_sem, self.recv_sem, self.used, self.sent = send_sem, recv_sem, 0, []

    def copy(self, src, dst, device):
        made = pltpu.make_async_remote_copy(
            src_ref=src,
            dst_ref=dst,
            send_sem=self.send_sem.at[self.used],
            recv_sem=self.recv_sem.at[self.used],
            device_id=device,
            device_id_type=MESH,
        )
        self.used += 1
        made.start()
        self.sent.append(made)
        return made

    def drain(self):
        for made in self.sent:
            made.wait_send()
        self.sent = []


def gather_kernel(dp_size, parts, count, *refs):
    shards, bias = refs[:count], refs[count]
    wholes, biases = refs[count + 1 : 2 * count + 1], refs[2 * count + 1]
    local_sem, send_sem, recv_sem = refs[2 * count + 2 :]
    here = Place(dp_size, parts)
    y, x, c = here.y, here.x, here.c
    locals_ = [
        pltpu.make_async_copy(shard, whole.at[0], local_sem.at[i])
        for i, (shard, whole) in enumerate(zip(shards, wholes))
    ] + [pltpu.make_async_copy(bias, biases.at[0], local_sem.at[count])]
    greet([here.flip(n) for n in "yxc"] + [here.shift(k) for k in range(1, parts)])
    link = Link(send_sem, recv_sem)
    along = []
    for i, (shard, whole) in enumerate(zip(shards, wholes)):
        along.append(
            [
                link.copy(shard.at[y, x, c], whole.at[parts - k, y, x, c], here.shift(k))
                for k in range(1, parts)
            ]
        )
        if i == 0:
            along[0] += [
                link.copy(bias, biases.at[parts - k], here.shift(k)) for k in range(1, parts)
            ]
    for made in locals_:
        made.start()
    away = pl.ds(1, parts - 1)
    first, second, third = {}, {}, {}
    for step in range(count + 3):
        if step < count:
            whole = wholes[step]
            half = whole.shape[4] // 2
            lo, hi = pl.ds(0, half), pl.ds(half, half)
            for made in along[step]:
                made.wait_recv()
            a, b = whole.at[away, y, x, c, lo], whole.at[away, y, x, c, hi]
            first[step] = [link.copy(a, a, here.flip("x")), link.copy(b, b, here.flip("y"))]
        if 0 <= step - 1 < count:
            whole = wholes[step - 1]
            half = whole.shape[4] // 2
            lo, hi = pl.ds(0, half), pl.ds(half, half)
            for made in first[step - 1]:
                made.wait_recv()
            a, b = whole.at[away, y, :, c, lo], whole.at[away, :, x, c, hi]
            second[step - 1] = [link.copy(a, a, here.flip("y")), link.copy(b, b, here.flip("x"))]
        if 0 <= step - 2 < count:
            whole = wholes[step - 2]
            for made in second[step - 2]:
                made.wait_recv()
            a = whole.at[away, :, :, c]
            third[step - 2] = [link.copy(a, a, here.flip("c"))]
        if 0 <= step - 3 < count:
            for made in third[step - 3]:
                made.wait_recv()
    link.drain()
    for made in locals_:
        made.wait()


def gather(shards, bias, dp_size, parts):
    shards = [s.reshape(2, 2, 2, s.shape[0] // FAN, s.shape[1]) for s in shards]
    count = len(shards)
    copies = count * (parts - 1 + 5) + parts - 1
    outs = pl.pallas_call(
        partial(gather_kernel, dp_size, parts, count),
        out_shape=[jax.ShapeDtypeStruct((parts,) + s.shape, s.dtype) for s in shards + [bias]],
        in_specs=[ANY] * (count + 1),
        out_specs=[ANY] * (count + 1),
        scratch_shapes=[
            pltpu.SemaphoreType.DMA((count + 1,)),
            pltpu.SemaphoreType.DMA((copies,)),
            pltpu.SemaphoreType.DMA((copies,)),
        ],
        compiler_params=pltpu.CompilerParams(collective_id=0, has_side_effects=True),
    )(*shards, bias)
    return [o.reshape(parts, -1, o.shape[-1]) for o in outs]


def add_into(target, other, lead):
    shape = other.shape[:lead]
    total = math.prod(shape)

    def body(i, carry):
        index = []
        for extent in reversed(shape):
            index.append(i % extent)
            i = i // extent
        index = tuple(reversed(index))
        target_i, other_i = target.at[index], other.at[index]
        target_i[...] = (target_i[...].astype(F32) + other_i[...].astype(F32)).astype(target.dtype)
        return carry

    lax.fori_loop(0, total, body, 0)


def reduce_kernel(dp_size, parts, count, *refs):
    grads, small = refs[:count], refs[count]
    outs, small_out = refs[count + 1 : 2 * count + 1], refs[2 * count + 1]
    rest = refs[2 * count + 2 :]
    get_c, get_y1, get_x2, get_x1, get_y2, get_z = [
        rest[i * count : (i + 1) * count] for i in range(6)
    ]
    small_acc, small_get, send_sem, recv_sem = rest[6 * count :]
    here = Place(dp_size, parts)
    y, x, c = here.y, here.x, here.c
    strides = [1 << b for b in range(dp_size.bit_length() - 1)]
    partners = [here.flip_stride(s) for s in strides]
    greet(partners + [here.shift(k) for k in range(1, parts)])
    link = Link(send_sem, recv_sem)
    stage = [{} for _ in range(4)]
    for i in range(count):
        stage[0][i] = [link.copy(grads[i].at[:, :, :, 1 - c], get_c[i], here.flip("c"))]

    small_acc[0] = small[...]
    rounds = partners + [
        (here.d, here.t + (1 << b) * (1 - 2 * ((here.t // (1 << b)) % 2)))
        for b in range(parts.bit_length() - 1)
    ]

    def small_round(r):
        return link.copy(small_acc.at[r], small_get.at[r], rounds[r])

    pending = small_round(0)
    done_rounds = 0

    def advance():
        nonlocal pending, done_rounds
        if pending is None:
            return
        pending.wait_recv()
        r = done_rounds
        small_acc[r + 1] = small_acc[r] + small_get[r]
        done_rounds += 1
        pending = small_round(done_rounds) if done_rounds < len(rounds) else None

    for step in range(count + 3):
        if step < count:
            g = grads[step]
            half = g.shape[4] // 2
            lo, hi = pl.ds(0, half), pl.ds(half, half)
            for made in stage[0][step]:
                made.wait_recv()
            add_into(g.at[:, :, :, c], get_c[step], 3)
            stage[1][step] = [
                link.copy(g.at[:, 1 - y, :, c, lo], get_y1[step], here.flip("y")),
                link.copy(g.at[:, :, 1 - x, c, hi], get_x1[step], here.flip("x")),
            ]
        if 0 <= step - 1 < count:
            i = step - 1
            g = grads[i]
            half = g.shape[4] // 2
            lo, hi = pl.ds(0, half), pl.ds(half, half)
            for made in stage[1][i]:
                made.wait_recv()
            add_into(g.at[:, y, :, c, lo], get_y1[i], 2)
            add_into(g.at[:, :, x, c, hi], get_x1[i], 2)
            stage[2][i] = [
                link.copy(g.at[:, y, 1 - x, c, lo], get_x2[i], here.flip("x")),
                link.copy(g.at[:, 1 - y, x, c, hi], get_y2[i], here.flip("y")),
            ]
        if 0 <= step - 2 < count:
            i = step - 2
            g = grads[i]
            half = g.shape[4] // 2
            lo, hi = pl.ds(0, half), pl.ds(half, half)
            for made in stage[2][i]:
                made.wait_recv()
            add_into(g.at[:, y, x, c, lo], get_x2[i], 1)
            add_into(g.at[:, y, x, c, hi], get_y2[i], 1)
            stage[3][i] = [
                link.copy(g.at[k, y, x, c], get_z[i].at[k - 1], here.shift(k))
                for k in range(1, parts)
            ]
        if 0 <= step - 3 < count:
            i = step - 3
            for made in stage[3][i]:
                made.wait_recv()
            total = grads[i][0, y, x, c].astype(F32)
            for k in range(parts - 1):
                total += get_z[i][k].astype(F32)
            outs[i][...] = total
        advance()
    while pending is not None:
        advance()
    small_out[...] = small_acc[len(rounds)]
    link.drain()


def reduce_all(grads, small, dp_size, parts):
    grads = [g.reshape(parts, 2, 2, 2, g.shape[1] // FAN, g.shape[2]) for g in grads]
    count = len(grads)
    rounds = dp_size.bit_length() - 1 + parts.bit_length() - 1
    copies = count * (5 + parts - 1) + rounds
    scratch = []
    for lead in ((parts, 2, 2), (parts, 2), (parts,), (parts, 2), (parts,), (parts - 1,)):
        for g in grads:
            rows = g.shape[4] // (1 if len(lead) == 3 or lead == (parts - 1,) else 2)
            scratch.append(pltpu.VMEM(lead + (rows, g.shape[5]), g.dtype))
    outs = pl.pallas_call(
        partial(reduce_kernel, dp_size, parts, count),
        out_shape=[jax.ShapeDtypeStruct(g.shape[4:], F32) for g in grads]
        + [jax.ShapeDtypeStruct(small.shape, F32)],
        in_specs=[VMEM] * (count + 1),
        out_specs=[VMEM] * (count + 1),
        scratch_shapes=scratch
        + [
            pltpu.VMEM((rounds + 1,) + small.shape, F32),
            pltpu.VMEM((rounds,) + small.shape, F32),
            pltpu.SemaphoreType.DMA((copies,)),
            pltpu.SemaphoreType.DMA((copies,)),
        ],
        input_output_aliases={},
        compiler_params=pltpu.CompilerParams(
            collective_id=1, has_side_effects=True, vmem_limit_bytes=63 * 1024 * 1024
        ),
    )(*grads, small)
    return outs[:count], outs[count]


def layer_norm(values, gain, shift):
    average = jnp.mean(values, axis=-1, keepdims=True)
    centered = values - average
    spread = jnp.mean(centered * centered, axis=-1, keepdims=True)
    return centered * lax.rsqrt(spread + 1e-06) * gain + shift


def gelu_exact(values):
    return jax.nn.gelu(values, approximate=False)


def dot(spec, a, b):
    return jnp.einsum(spec, a, b, preferred_element_type=F32)


def attend_forward(q, k, v, labels, scale):
    scores = dot("hqd,hkd->hqk", q, k) * scale
    scores = jnp.where((labels[:, None] == labels[None, :])[None], scores, -1e30)
    highest = jnp.max(scores, axis=-1, keepdims=True)
    expon = jnp.exp(scores - highest)
    totals = jnp.sum(expon, axis=-1, keepdims=True)
    weights = (expon / totals).astype(BF16)
    return dot("hqk,hkd->hqd", weights, v).astype(BF16), highest + jnp.log(totals)


def attend_backward(q, k, v, labels, log_totals, g, scale):
    scores = dot("hqd,hkd->hqk", q, k) * scale
    scores = jnp.where((labels[:, None] == labels[None, :])[None], scores, -1e30)
    weights = jnp.exp(scores - log_totals)
    gv = dot("hqk,hqd->hkd", weights.astype(BF16), g).astype(BF16)
    gw = dot("hqd,hkd->hqk", g, v)
    inner = jnp.sum(gw * weights, axis=-1, keepdims=True)
    gs = (weights * (gw - inner)).astype(BF16)
    gq = (dot("hqk,hkd->hqd", gs, k) * scale).astype(BF16)
    gk = (dot("hqk,hqd->hkd", gs, q) * scale).astype(BF16)
    return gq, gk, gv


def unroll_parts(pieces, tensor_index):
    return jnp.roll(pieces, tensor_index, axis=0).reshape(-1)


def on_device(dp_size, parts, tokens, segments, cotangent, ln1_gain, ln1_bias, w_qkv, q_bias, v_bias, w_out, out_bias, ln2_gain, ln2_bias, w_fc1, fc1_bias, w_fc2, fc2_bias):
    tensor_index = lax.axis_index("tensor")
    rows = tokens.shape[0]
    width = tokens.shape[1]
    scale = 1.0 / math.sqrt(HD)
    head_cols = w_out.shape[0]
    heads = head_cols // HD
    hidden_cols = w_fc1.shape[1]
    positions = jnp.arange(segments.shape[0]) % SEQ
    earlier = jnp.concatenate([jnp.full((1,), -2, jnp.int32), segments[:-1]])
    first_all = ((segments >= 0) & ((positions == 0) | (segments != earlier))).astype(F32)
    first_rows = lax.dynamic_slice_in_dim(first_all, tensor_index * rows, rows)
    labels = lax.dynamic_slice_in_dim(segments, tensor_index * rows, rows)
    live = (labels >= 0).astype(F32)

    out_rows = -(-head_cols // (32 * FAN)) * 32 * FAN
    out_padded = jnp.pad(w_out, ((0, out_rows - head_cols), (0, 0)))
    bias = jnp.zeros((16, max(2 * head_cols, hidden_cols)), BF16)
    bias = bias.at[0, :head_cols].set(q_bias).at[1, :head_cols].set(v_bias)
    bias = bias.at[2, :hidden_cols].set(fc1_bias)
    full_qkv, full_out, full_fc1, full_fc2, full_bias = gather(
        [w_qkv, out_padded, w_fc1, w_fc2], bias, dp_size, parts
    )
    full_out = full_out[:, :head_cols]
    full_bias = full_bias.astype(F32)
    bias_q, bias_v, bias_1 = full_bias[:, 0, :head_cols], full_bias[:, 1, :head_cols], full_bias[:, 2, :hidden_cols]

    inputs_f = tokens.astype(F32)
    normed, norm1_back = jax.vjp(layer_norm, inputs_f, ln1_gain.astype(F32), ln1_bias.astype(F32))
    normed_low = normed.astype(BF16)
    blocks = rows // SEQ
    mixed = dot("nd,kdm->knm", normed_low, full_qkv).reshape(parts, blocks, SEQ, heads, 3, HD)
    mixed = jnp.transpose(mixed, (4, 1, 0, 3, 2, 5)).reshape(3, blocks, parts * heads, SEQ, HD)
    q = (mixed[0] + bias_q.reshape(1, parts * heads, 1, HD)).astype(BF16)
    k = mixed[1].astype(BF16)
    v = (mixed[2] + bias_v.reshape(1, parts * heads, 1, HD)).astype(BF16)
    label_blocks = labels.reshape(blocks, SEQ)
    attended, log_totals = jax.vmap(partial(attend_forward, scale=scale))(q, k, v, label_blocks)
    heads_out = attended.reshape(blocks, parts, heads, SEQ, HD).transpose(1, 0, 3, 2, 4).reshape(parts, rows, head_cols)
    resid = inputs_f + dot("knm,kmd->nd", heads_out, full_out) + out_bias.astype(F32)
    normed2, norm2_back = jax.vjp(layer_norm, resid, ln2_gain.astype(F32), ln2_bias.astype(F32))
    normed2_low = normed2.astype(BF16)
    hidden = dot("nd,kdm->knm", normed2_low, full_fc1) + bias_1[:, None, :]
    active, gelu_back = jax.vjp(gelu_exact, hidden)
    active_low = active.astype(BF16)
    output = (resid + dot("knm,kmd->nd", active_low, full_fc2) + fc2_bias.astype(F32)).astype(BF16)
    out_values = output.astype(F32)
    first_col = first_rows[:, None]

    grad_out = cotangent.astype(F32) * live[:, None]
    grad_branch = grad_out.astype(BF16)
    grad_fc2 = dot("nd,knm->kdm", grad_branch, active_low).astype(BF16)
    grad_hidden = gelu_back(dot("nd,kmd->knm", grad_branch, full_fc2))[0].astype(BF16)
    grad_fc1 = dot("nd,knm->kdm", normed2_low, grad_hidden).astype(BF16)
    grad_normed2 = dot("knm,kdm->nd", grad_hidden, full_fc1)
    grad_resid_norm, grad_ln2_gain, grad_ln2_bias = norm2_back(grad_normed2)
    grad_resid = grad_out + grad_resid_norm
    grad_attn = grad_resid.astype(BF16)
    grad_w_out = dot("nd,knm->kdm", grad_attn, heads_out).astype(BF16)
    grad_heads = dot("nd,kmd->knm", grad_attn, full_out).astype(BF16)
    grad_heads = grad_heads.reshape(parts, blocks, SEQ, heads, HD).transpose(1, 0, 3, 2, 4).reshape(blocks, parts * heads, SEQ, HD)
    gq, gk, gv = jax.vmap(partial(attend_backward, scale=scale))(q, k, v, label_blocks, log_totals, grad_heads)
    stacked = jnp.stack([gq, gk, gv]).reshape(3, blocks, parts, heads, SEQ, HD)
    grad_mixed = jnp.transpose(stacked, (2, 1, 4, 3, 0, 5)).reshape(parts, rows, heads * 3 * HD)
    grad_w_qkv = dot("nd,knm->kdm", normed_low, grad_mixed).astype(BF16)
    grad_normed = dot("knm,kdm->nd", grad_mixed, full_qkv)
    grad_inputs_norm, grad_ln1_gain, grad_ln1_bias = norm1_back(grad_normed)
    grad_tokens = (grad_resid + grad_inputs_norm).astype(BF16)

    sums_q = jnp.sum(gq.astype(F32), axis=(0, 2)).reshape(parts, head_cols)
    sums_v = jnp.sum(gv.astype(F32), axis=(0, 2)).reshape(parts, head_cols)
    sums_1 = jnp.sum(grad_hidden.astype(F32), axis=1)
    pieces = [
        grad_ln1_gain,
        grad_ln1_bias,
        unroll_parts(sums_q, tensor_index),
        unroll_parts(sums_v, tensor_index),
        jnp.sum(grad_resid, axis=0),
        unroll_parts(sums_1, tensor_index),
        jnp.sum(grad_out, axis=0),
        grad_ln2_gain,
        grad_ln2_bias,
        jnp.sum(first_col * out_values, axis=0),
        jnp.sum(first_col * out_values * out_values, axis=0),
        jnp.full((width,), jnp.sum(first_rows)),
    ]
    sizes = [p.shape[0] for p in pieces]
    flat = jnp.concatenate(pieces)
    lines = -(-flat.shape[0] // (8 * width)) * 8
    flat = jnp.pad(flat, (0, lines * width - flat.shape[0])).reshape(lines, width)
    (sum_qkv, sum_out, sum_fc1, sum_fc2), small = reduce_all(
        [grad_w_qkv, grad_w_out, grad_fc1, grad_fc2], flat, dp_size, parts
    )
    low = dp_size // FAN

    def finish(array):
        if low == 1:
            return array
        groups = [[i * low + j for j in range(low)] for i in range(FAN)]
        return lax.psum_scatter(array, "dp", scatter_dimension=0, axis_index_groups=groups, tiled=True)

    sum_qkv, sum_out, sum_fc1, sum_fc2 = (finish(a) for a in (sum_qkv, sum_out, sum_fc1, sum_fc2))
    small = small.reshape(-1)
    totals, at = [], 0
    for size in sizes:
        totals.append(small[at : at + size])
        at += size
    count = totals[11]
    cls_mean = totals[9] / count
    cls_spread = totals[10] / count - cls_mean * cls_mean
    cls_features = first_col * (out_values - cls_mean) * lax.rsqrt(cls_spread + 1e-05)
    return (output, grad_tokens, cls_features, sum_qkv, totals[2], totals[3], sum_out.T, totals[4], sum_fc1, totals[5], sum_fc2.T, totals[6], totals[0], totals[1], totals[7], totals[8])


def solution(mesh):
    dp_size, parts = mesh.shape["dp"], mesh.shape["tensor"]
    row, whole, cols, out_cols = P(("dp", "tensor"), None), P(), P(None, "tensor"), P("tensor")
    down = P("tensor", None)
    in_specs = (row, P("dp"), row, whole, whole, cols, out_cols, out_cols, down, whole, whole, whole, cols, out_cols, down, whole)
    spread, turned = P("dp", "tensor"), P("tensor", "dp")
    out_specs = (row, row, row, spread, whole, whole, turned, whole, spread, whole, turned, whole, whole, whole, whole, whole)
    return jax.shard_map(partial(on_device, dp_size, parts), mesh=mesh, in_specs=in_specs, out_specs=out_specs, check_vma=False)
```

```python
from functools import partial
import math

import jax
import jax.numpy as jnp
from jax import lax
from jax.experimental import pallas as pl
from jax.experimental.pallas import tpu as pltpu
from jax.sharding import PartitionSpec as P

HD = 64
SEQ = 512
FAN = 8
F32 = jnp.float32
BF16 = jnp.bfloat16
MESH = pl.DeviceIdType.MESH
ANY = pl.BlockSpec(memory_space=pl.ANY)
VMEM = pl.BlockSpec(memory_space=pltpu.VMEM)


def mm(a, b):
    return lax.dot_general(a, b, (((1,), (0,)), ((), ())), preferred_element_type=F32)


def mm_nt(a, b):
    return lax.dot_general(a, b, (((1,), (1,)), ((), ())), preferred_element_type=F32)


def mm_tn(a, b):
    return lax.dot_general(a, b, (((0,), (0,)), ((), ())), preferred_element_type=F32)


class Place:
    def __init__(self, dp_size, parts):
        self.d = lax.axis_index("dp")
        self.t = lax.axis_index("tensor")
        self.dp_size, self.parts = dp_size, parts
        self.low = dp_size // FAN
        block = self.d // self.low
        self.y, self.x, self.c = block // 4, (block // 2) % 2, block % 2

    def flip(self, name):
        stride = self.low * {"y": 4, "x": 2, "c": 1}[name]
        bit = {"y": self.y, "x": self.x, "c": self.c}[name]
        return (self.d + stride * (1 - 2 * bit), self.t)

    def flip_stride(self, stride):
        bit = (self.d // stride) % 2
        return (self.d + stride * (1 - 2 * bit), self.t)

    def shift(self, k):
        return (self.d, (self.t + k) % self.parts)


def greet(partners):
    barrier = pltpu.get_barrier_semaphore()
    for partner in partners:
        pl.semaphore_signal(barrier, inc=1, device_id=partner, device_id_type=MESH)
    pl.semaphore_wait(barrier, len(partners))


class Link:
    def __init__(self, send_sem, recv_sem):
        self.send_sem, self.recv_sem, self.used = send_sem, recv_sem, 0

    def copy(self, src, dst, device):
        made = pltpu.make_async_remote_copy(
            src_ref=src,
            dst_ref=dst,
            send_sem=self.send_sem.at[self.used],
            recv_sem=self.recv_sem.at[self.used],
            device_id=device,
            device_id_type=MESH,
        )
        self.used += 1
        return made


def start(copies):
    for made in copies:
        made.start()


def arrive(copies):
    for made in copies:
        made.wait_recv()


def left(copies):
    for made in copies:
        made.wait_send()


def loop(count, body, hooks=None):
    def step(i, carry):
        for at, hook in (hooks or {}).items():
            pl.when(i == at)(hook)
        body(i)
        return carry

    lax.fori_loop(0, count, step, 0)


def add_into(target, other, lead):
    shape = other.shape[:lead]

    def body(i):
        index = []
        for extent in reversed(shape):
            index.append(i % extent)
            i = i // extent
        index = tuple(reversed(index))
        target_i, other_i = target.at[index], other.at[index]
        target_i[...] = (target_i[...].astype(F32) + other_i[...].astype(F32)).astype(target.dtype)

    loop(math.prod(shape), body)


def gather_unit(here, link, shard, whole):
    parts = here.parts
    y, x, c = here.y, here.x, here.c
    away = pl.ds(1, parts - 1)
    half = whole.shape[4] // 2
    lo, hi = pl.ds(0, half), pl.ds(half, half)
    along = [
        link.copy(shard.at[y, x, c], whole.at[parts - k, y, x, c], here.shift(k))
        for k in range(1, parts)
    ]
    a, b = whole.at[away, y, x, c, lo], whole.at[away, y, x, c, hi]
    first = [link.copy(a, a, here.flip("x")), link.copy(b, b, here.flip("y"))]
    a, b = whole.at[away, y, :, c, lo], whole.at[away, :, x, c, hi]
    second = [link.copy(a, a, here.flip("y")), link.copy(b, b, here.flip("x"))]
    a = whole.at[away, :, :, c]
    third = [link.copy(a, a, here.flip("c"))]
    return [along, first, second, third]


class Reduction:
    def __init__(self, here, link, grad, first, many, got, got_z):
        self.here, self.got = here, got
        got_c, got_y1, got_x2, got_x1, got_y2 = got
        y, x, c = here.y, here.x, here.c
        half = grad.shape[4] // 2
        self.lo, self.hi = lo, hi = pl.ds(0, half), pl.ds(half, half)
        self.grad = g = grad.at[pl.ds(first, many)]
        self.stages = [
            [link.copy(g.at[:, :, :, 1 - c], got_c, here.flip("c"))],
            [
                link.copy(g.at[:, 1 - y, :, c, lo], got_y1, here.flip("y")),
                link.copy(g.at[:, :, 1 - x, c, hi], got_x1, here.flip("x")),
            ],
            [
                link.copy(g.at[:, y, 1 - x, c, lo], got_x2, here.flip("x")),
                link.copy(g.at[:, 1 - y, x, c, hi], got_y2, here.flip("y")),
            ],
            [
                link.copy(grad.at[k, y, x, c], got_z.at[k - 1], here.shift(k))
                for k in range(first, first + many)
                if k > 0
            ],
        ]

    def step(self, s):
        y, x, c = self.here.y, self.here.x, self.here.c
        g, lo, hi = self.grad, self.lo, self.hi
        got_c, got_y1, got_x2, got_x1, got_y2 = self.got
        if s > 0:
            arrive(self.stages[s - 1])
        if s == 1:
            add_into(g.at[:, :, :, c], got_c, 3)
        if s == 2:
            add_into(g.at[:, y, :, c, lo], got_y1, 2)
            add_into(g.at[:, :, x, c, hi], got_x1, 2)
        if s == 3:
            add_into(g.at[:, y, x, c, lo], got_x2, 1)
            add_into(g.at[:, y, x, c, hi], got_y2, 1)
        if s < 4:
            start(self.stages[s])

    def drain(self):
        for copies in self.stages:
            left(copies)


def normalize(values):
    average = jnp.mean(values, axis=-1, keepdims=True)
    centered = values - average
    spread = jnp.mean(centered * centered, axis=-1, keepdims=True)
    scale = lax.rsqrt(spread + 1e-06)
    return centered * scale, scale


def normalize_back(hat, scale, gain, grad):
    scaled = grad * gain
    return (
        scaled
        - jnp.mean(scaled, axis=-1, keepdims=True)
        - hat * jnp.mean(scaled * hat, axis=-1, keepdims=True)
    ) * scale


ROWS = 64
UNITS = 5
NAMES = (
    "tokens",
    "cot",
    "segments",
    "vecs",
    "bias",
    "w_qkv",
    "w_out",
    "w_fc1",
    "w_fc2",
)
OUTS = (
    "output",
    "g_tokens",
    "s_qkv",
    "s_out",
    "s_fc1",
    "s_fc2",
    "small",
    "late",
    "cls",
)
SCRATCH = (
    "f_qkv",
    "f_out",
    "f_fc1",
    "f_fc2",
    "biases",
    "normed",
    "mixed",
    "mask",
    "lse",
    "heads",
    "resid",
    "normed2",
    "active",
    "slope",
    "turned",
    "acc",
    "tile",
    "g_low",
    "g_heads",
    "g_fc2",
    "g_out",
    "cols",
    "sums",
    "got_small",
    "late_sums",
    "got_late",
)


def layer_kernel(dp_size, parts, heads, *refs):
    refs = list(refs)
    ref = {}
    for name in NAMES + OUTS + SCRATCH:
        ref[name] = refs.pop(0)
    got = [[refs.pop(0) for _ in range(5)] for _ in range(UNITS + parts)]
    got_z = [refs.pop(0) for _ in range(UNITS + 1)]
    local_sem, send_sem, recv_sem = refs
    tokens, cot, cols, vecs = ref["tokens"], ref["cot"], ref["cols"], ref["vecs"]
    segments = ref["segments"]
    f_qkv, f_out, f_fc1, f_fc2 = ref["f_qkv"], ref["f_out"], ref["f_fc1"], ref["f_fc2"]
    biases, normed, mixed, mask = ref["biases"], ref["normed"], ref["mixed"], ref["mask"]
    lse, hd, resid, normed2 = ref["lse"], ref["heads"], ref["resid"], ref["normed2"]
    active, slope, turned, acc = ref["active"], ref["slope"], ref["turned"], ref["acc"]
    tile, g_low, g_heads, sums = ref["tile"], ref["g_low"], ref["g_heads"], ref["sums"]
    g_fc2, g_out = ref["g_fc2"], ref["g_out"]
    g_mixed = active
    wide = f_qkv.shape[5]
    g_qkv = f_fc1.at[:, :, :, :, :, pl.ds(0, wide)]
    g_fc1 = f_fc2
    width = tokens.shape[1]
    small, late = sums.at[0], ref["late_sums"].at[0]
    here = Place(dp_size, parts)
    qk_wide = heads * 128
    strides = [1 << b for b in range(dp_size.bit_length() - 1)]
    bits = [here.flip_stride(s) for s in strides]
    link = Link(send_sem, recv_sem)

    shards = [ref[n] for n in ("w_qkv", "w_out", "w_fc1", "w_fc2")]
    wholes = [f_qkv, f_out, f_fc1, f_fc2]
    own = [
        pltpu.make_async_copy(a, b.at[0], local_sem.at[i])
        for i, (a, b) in enumerate(zip(shards + [ref["bias"]], wholes + [biases]))
    ]
    start(own)
    greet(bits + [here.shift(k) for k in range(1, parts)])
    def columns(array, first, many):
        return array.at[:, :, :, :, pl.ds(first, many)] if len(array.shape) == 5 else array.at[:, :, :, :, :, pl.ds(first, many)]

    cut = f_fc1.shape[5] // 2
    plans = {"q": gather_unit(here, link, shards[0], f_qkv), "o": gather_unit(here, link, shards[1], f_out)}
    for name, i, first in (("a", 2, 0), ("b", 2, cut), ("c", 3, 0), ("d", 3, cut)):
        plans[name] = gather_unit(
            here, link, columns(shards[i], first, cut), columns(wholes[i], first, cut)
        )
    plans["q"][0] += [
        link.copy(ref["bias"], biases.at[parts - k], here.shift(k)) for k in range(1, parts)
    ]
    for plan in plans.values():
        start(plan[0])
    units = {}
    for i, (name, grad) in enumerate(
        (
            ("A", columns(g_fc2, 0, cut)),
            ("B", columns(g_fc2, cut, cut)),
            ("C", columns(g_fc1, 0, cut)),
            ("D", columns(g_fc1, cut, cut)),
            ("O", g_out),
        )
    ):
        units[name] = Reduction(here, link, grad, 0, parts, got[i], got_z[i])
    for k in range(parts):
        units[k] = Reduction(here, link, g_qkv, k, 1, got[UNITS + k], got_z[UNITS])

    def fwd(*steps):
        def run():
            for name, s in steps:
                arrive(plans[name][s])
                if s < 3:
                    start(plans[name][s + 1])

        return run

    def red(*steps):
        def run():
            for name, s in steps:
                units[name].step(s)

        return run

    def total(grad, got_last, out):
        value = grad[0, here.y, here.x, here.c].astype(F32)
        for k in range(parts - 1):
            value += got_last[k].astype(F32)
        out[...] = value

    tensor_bits = [
        (here.d, here.t + (1 << b) * (1 - 2 * ((here.t // (1 << b)) % 2)))
        for b in range(parts.bit_length() - 1)
    ]

    def butterfly(slots, got_slots):
        trips = [
            link.copy(slots.at[r], got_slots.at[r], partner)
            for r, partner in enumerate(bits + tensor_bits)
        ]

        def run(r):
            if r > 0:
                arrive([trips[r - 1]])
                slots[r] = slots[r - 1] + got_slots[r - 1]
            if r < len(trips):
                start([trips[r]])

        return trips, run

    trips, early_round = butterfly(sums, ref["got_small"])
    late_trips, late_round = butterfly(ref["late_sums"], ref["got_late"])

    def gain(i):
        return vecs[pl.ds(i, 1), :]

    chunks = SEQ // ROWS

    def rows_of(i):
        return pl.ds(pl.multiple_of(i * ROWS, ROWS), ROWS)

    small[...] = jnp.zeros_like(small)
    late[...] = jnp.zeros_like(late)
    labels = segments[pl.ds(here.t, 1), :]
    spot = lax.broadcasted_iota(jnp.int32, (1, SEQ), 1)
    earlier = pltpu.roll(labels, 1, 1)
    begins = (labels >= 0) & ((spot == 0) | (labels != earlier))
    line = labels.astype(F32)
    kinds = lax.broadcasted_iota(jnp.int32, (8, SEQ), 0)
    stacked = jnp.where(kinds == 0, line, jnp.where(kinds == 1, (labels >= 0).astype(F32), begins.astype(F32)))
    cols[...] = stacked.T

    def norm_one(i):
        r = rows_of(i)
        hat, _ = normalize(tokens[r, :].astype(F32))
        normed[r, :] = (hat * gain(0) + gain(1)).astype(BF16)
        mask[r, :] = jnp.where(cols[r, 0:1] == line, 0.0, -1e30)

    loop(chunks, norm_one)

    low_half = lax.broadcasted_iota(jnp.int32, (SEQ, 128), 1) < 64

    def qkv_part(k):
        for at in range(0, wide, 256):
            size = min(256, wide - at)
            w = f_qkv[k, :, :, :, :, pl.ds(at, size)].reshape(width, size)
            out = mm(normed[...], w) + biases[k, 0:1, pl.ds(at, size)].astype(F32)
            mixed[k, :, pl.ds(at, size)] = out.astype(BF16)

    def head_place(i):
        k, j = i // heads, i % heads
        at = pl.ds(pl.multiple_of(j * 128, 128), 128)
        v_at = pl.ds(pl.multiple_of(qk_wide + (j // 2) * 128, 128), 128)
        h_at = pl.ds(pl.multiple_of((j // 2) * 128, 128), 128)
        even = j % 2 == 0
        return k, at, v_at, h_at, even

    def scores_of(k, at):
        qk = mixed[k, :, at].astype(F32)
        q = jnp.where(low_half, qk * (1.0 / math.sqrt(HD)), 0.0).astype(BF16)
        kq = pltpu.roll(qk, 64, 1).astype(BF16)
        return mm_nt(kq, q) + mask[...], kq

    def mine_of(even):
        return low_half == even

    def attend(i):
        k, at, v_at, h_at, even = head_place(i)
        scores, _ = scores_of(k, at)
        highest = jnp.max(scores, axis=0, keepdims=True)
        expon = jnp.exp(scores - highest)
        total = jnp.sum(expon, axis=0, keepdims=True)
        lse[i, 0:1, :] = highest + jnp.log(total)
        weights = (expon * (1.0 / total)).astype(BF16)
        out = mm_tn(weights, mixed[k, :, v_at])
        before = jnp.where(even, 0.0, hd[k, :, h_at].astype(F32))
        hd[k, :, h_at] = jnp.where(mine_of(even), out, before).astype(BF16)

    own[0].wait()
    own[4].wait()
    qkv_part(0)
    loop(heads, attend)
    fwd(("q", 0), ("o", 0), ("q", 1), ("a", 0), ("o", 1), ("q", 2), ("b", 0), ("a", 1), ("q", 3))()
    loop(parts - 1, lambda k: qkv_part(k + 1))
    loop(
        heads * (parts - 1),
        lambda i: attend(i + heads),
        {
            1: fwd(("o", 2), ("c", 0)),
            2: fwd(("b", 1)),
            3: fwd(("a", 2)),
            4: fwd(("d", 0), ("o", 3)),
            5: fwd(("c", 1)),
            7: fwd(("b", 2), ("a", 3)),
            8: fwd(("d", 1)),
        },
    )
    for made in own[1:4]:
        made.wait()

    def project(n):
        at = pl.ds(pl.multiple_of(n * 256, 256), 256)
        total = tokens[:, at].astype(F32) + vecs[2:3, at]
        for k in range(parts):
            total += mm(hd[k], f_out[k, :, :, :, :, at].reshape(-1, 256))
        resid[:, at] = total

    loop(width // 256, project)

    def norm_two(i):
        r = rows_of(i)
        hat, _ = normalize(resid[r, :])
        normed2[r, :] = (hat * gain(3) + gain(4)).astype(BF16)

    loop(chunks, norm_two)
    hid = f_fc1.shape[5]
    tiles = hid // 256

    def fc1_tile(i):
        k, n = i // tiles, i % tiles
        at = pl.ds(pl.multiple_of(n * 256, 256), 256)
        tile[...] = mm(normed2[...], f_fc1[k, :, :, :, :, at].reshape(width, 256)) + biases[
            k, 1:2, at
        ].astype(F32)

        def gelu(j):
            r = rows_of(j)
            v = tile[r, :]
            cdf = 0.5 * (1.0 + lax.erf(v * (1.0 / math.sqrt(2.0))))
            pdf = jnp.exp(-0.5 * v * v) * (1.0 / math.sqrt(2.0 * math.pi))
            active[k, r, at] = (v * cdf).astype(BF16)
            slope[k, r, at] = (cdf + v * pdf).astype(BF16)

        loop(chunks, gelu)

    loop(tiles, fc1_tile)
    fwd(("c", 2), ("b", 3))()
    loop(
        tiles * (parts - 1),
        lambda i: fc1_tile(i + tiles),
        {2: fwd(("d", 2)), 4: fwd(("c", 3))},
    )

    def grad_branch(i):
        r = rows_of(i)
        g_low[r, :] = (cot[r, :].astype(F32) * cols[r, 1:2]).astype(BF16)

    loop(chunks, grad_branch)
    ones = jnp.ones((8, SEQ), BF16)

    def turn(source):
        def body(n):
            at = pl.ds(pl.multiple_of(n * 256, 256), 256)
            turned[at, :] = source[:, at].astype(F32).T.astype(BF16)

        loop(width // 256, body)

    def weight_grad(target, source, columns, parts_here=parts):
        def body(k):
            for at in range(0, columns, 256):
                size = min(256, columns - at)
                out = mm(turned[...], source[k, :, pl.ds(at, size)])
                target[k, :, :, :, :, pl.ds(at, size)] = out.astype(BF16).reshape(
                    2, 2, 2, width // FAN, size
                )

        return body

    turn(g_low)
    small[1:2, :] = mm(ones, g_low[...])[0:1]
    loop(parts, weight_grad(g_fc2, active, hid))
    red(("A", 0), ("B", 0))()
    fwd(("d", 3))()
    for plan in plans.values():
        for copies in plan:
            left(copies)

    def finish(n):
        at = pl.ds(pl.multiple_of(n * 256, 256), 256)
        total = resid[:, at] + vecs[5:6, at]
        for k in range(parts):
            total += mm(active[k], f_fc2[k, :, :, :, :, at].reshape(hid, 256))
        out = total.astype(BF16)
        ref["output"][:, at] = out
        values = out.astype(F32)
        picked = values * cols[:, 2:3]
        small[4:5, at] = jnp.sum(picked, axis=0, keepdims=True)
        small[5:6, at] = jnp.sum(picked * values, axis=0, keepdims=True)

    loop(width // 256, finish, {2: red(("A", 1))})
    red(("B", 1))()
    small[6:7, :] = jnp.broadcast_to(jnp.sum(cols[:, 2:3], axis=0, keepdims=True), (1, width))
    side = hid // 2

    def hidden_back(i):
        k, s = i // 2, i % 2
        at = pl.ds(pl.multiple_of(s * side, 128), side)
        back = mm_nt(g_low[...], f_fc2[k, s].reshape(side, width))
        back = (back * slope[k, :, at].astype(F32)).astype(BF16)
        slope[k, :, at] = back
        row = pl.ds(8 + (here.t + k) % parts, 1)
        small[row, at] = mm(ones, back)[0:1]

    loop(2 * parts, hidden_back, {6: red(("A", 2))})
    turn(normed2)
    loop(parts, weight_grad(g_fc1, slope, hid))
    red(("C", 0), ("D", 0), ("B", 2))()

    def normed2_back(s):
        at = pl.ds(pl.multiple_of(s * side, 128), side)
        total = mm_nt(slope[0], f_fc1[0, s].reshape(side, hid))
        for k in range(1, parts):
            total += mm_nt(slope[k], f_fc1[k, s].reshape(side, hid))
        acc[:, at] = total

    loop(2, normed2_back, {1: red(("C", 1))})
    red(("D", 1), ("A", 3))()

    def norm_two_back(i):
        r = rows_of(i)
        grad = acc[r, :]
        hat, scale = normalize(resid[r, :])
        back = cot[r, :].astype(F32) * cols[r, 1:2] + normalize_back(hat, scale, gain(3), grad)
        acc[r, :] = back
        g_low[r, :] = back.astype(BF16)
        small[2:3, :] += jnp.sum(grad * hat, axis=0, keepdims=True)
        small[3:4, :] += jnp.sum(grad, axis=0, keepdims=True)
        small[0:1, :] += jnp.sum(back, axis=0, keepdims=True)

    loop(chunks, norm_two_back)
    turn(g_low)
    v_wide = hd.shape[2]
    loop(parts, weight_grad(g_out, hd, v_wide))
    red(("O", 0), ("B", 3))()
    early_round(0)

    def heads_back(k):
        g_heads[k] = mm_nt(g_low[...], f_out[k].reshape(v_wide, width)).astype(BF16)

    loop(parts, heads_back)

    def attend_back(i):
        k, at, v_at, h_at, even = head_place(i)
        mine = mine_of(even)
        scores, kq = scores_of(k, at)
        weights = jnp.exp(scores - lse[i, 0:1, :])
        grad = g_heads[k, :, h_at]
        own_grad = jnp.where(mine, grad.astype(F32), 0.0).astype(BF16)
        g_value = mm(weights.astype(BF16), grad)
        g_weights = mm_nt(mixed[k, :, v_at], own_grad)
        inner = jnp.sum(g_weights * weights, axis=0, keepdims=True)
        g_scores = (weights * (g_weights - inner)).astype(BF16)
        g_q = mm_tn(g_scores, kq)
        g_k = mm(g_scores, kq)
        both = jnp.where(low_half, g_q, g_k) * (1.0 / math.sqrt(HD))
        g_mixed[k, :, at] = both.astype(BF16)
        before = jnp.where(even, 0.0, g_mixed[k, :, v_at].astype(F32))
        g_mixed[k, :, v_at] = jnp.where(mine, g_value, before).astype(BF16)

    turn(normed)

    def qkv_grad(k):
        def run():
            weight_grad(g_qkv, g_mixed, wide)(k)
            units[k].step(0)
            row = pl.ds(2 + (here.t + k) % parts, 1)
            late[row, pl.ds(0, wide)] = mm(ones, g_mixed[k, :, pl.ds(0, wide)])[0:1]

        return run

    hooks = {}

    def hook(at, *runs):
        hooks.setdefault(at, []).extend(runs)

    for k in range(1, parts):
        hook(heads * k, qkv_grad(k - 1))
    hook(1, red(("C", 2)))
    hook(2, red(("O", 1)))
    hook(5, red(("D", 2)))
    hook(7, red((0, 1)))
    hook(8, red(("A", 4), ("C", 3)))
    hook(9, red((1, 1)))
    hook(10, red(("O", 2)))
    hook(11, red(("D", 3), (0, 2)))
    for r in range(1, len(trips) + 1):
        hook(min(2 * r, heads * parts - 1), partial(early_round, r))

    def joined(runs):
        def run():
            for one in runs:
                one()

        return run

    loop(heads * parts, attend_back, {at: joined(runs) for at, runs in hooks.items()})
    qkv_grad(parts - 1)()
    for k in range(2, parts - 1):
        red((k, 1))()

    def normed_back(s):
        at = pl.ds(pl.multiple_of(s * side, 128), side)
        total = mm_nt(g_mixed[0, :, pl.ds(0, wide)], f_qkv[0, s].reshape(side, wide))
        for k in range(1, parts):
            total += mm_nt(g_mixed[k, :, pl.ds(0, wide)], f_qkv[k, s].reshape(side, wide))
        tile_out = total
        resid[:, at] = tile_out

    loop(2, normed_back, {1: red((parts - 1, 1), (1, 2), ("O", 3))})

    def norm_one_back(i):
        r = rows_of(i)
        grad = resid[r, :]
        hat, scale = normalize(tokens[r, :].astype(F32))
        back = acc[r, :] + normalize_back(hat, scale, gain(0), grad)
        ref["g_tokens"][r, :] = back.astype(BF16)
        late[0:1, :] += jnp.sum(grad * hat, axis=0, keepdims=True)
        late[1:2, :] += jnp.sum(grad, axis=0, keepdims=True)

    loop(chunks, norm_one_back)
    late_round(0)
    for k in range(2, parts):
        red((k, 2))()
    late_round(1)
    for k in range(parts):
        red((k, 3))()
    late_round(2)
    final = sums.at[len(trips)]
    mean = final[4:5, :] / final[6:7, :]
    spread = final[5:6, :] / final[6:7, :] - mean * mean
    spread = lax.rsqrt(spread + 1e-05)

    def features(i):
        r = rows_of(i)
        ref["cls"][r, :] = cols[r, 2:3] * (ref["output"][r, :].astype(F32) - mean) * spread

    loop(chunks, features)
    late_round(3)
    red(("B", 4), ("C", 4), ("D", 4), ("O", 4))()
    total(columns(g_fc2, 0, cut), got_z[0], ref["s_fc2"].at[:, pl.ds(0, cut)])
    total(columns(g_fc2, cut, cut), got_z[1], ref["s_fc2"].at[:, pl.ds(cut, cut)])
    total(columns(g_fc1, 0, cut), got_z[2], ref["s_fc1"].at[:, pl.ds(0, cut)])
    total(columns(g_fc1, cut, cut), got_z[3], ref["s_fc1"].at[:, pl.ds(cut, cut)])
    total(g_out, got_z[4], ref["s_out"])
    for r in range(4, len(late_trips) + 1):
        late_round(r)
    for k in range(parts):
        red((k, 4))()
    total(g_qkv, got_z[UNITS], ref["s_qkv"])
    ref["small"][...] = final[...]
    ref["late"][...] = ref["late_sums"][len(late_trips)]
    left(trips + late_trips)
    for unit in units.values():
        unit.drain()


def layer(tokens, cot, segments, vecs, bias, shards, dp_size, parts, heads):
    shards = [s.reshape(2, 2, 2, s.shape[0] // FAN, s.shape[1]) for s in shards]
    width, hid = tokens.shape[1], shards[2].shape[4]
    wide, v_wide = shards[0].shape[4], FAN * shards[1].shape[3]
    lines, late_lines = -(-(8 + parts) // 8) * 8, -(-(2 + parts) // 8) * 8
    rounds = dp_size.bit_length() - 1 + parts.bit_length() - 1
    copies = 6 * (5 + parts - 1) + parts - 1 + (UNITS + parts) * (5 + parts) + 2 * rounds
    blk = width // FAN
    grads = [(blk, wide), (blk, v_wide), (blk, hid), (blk, hid)]
    whole = [pltpu.VMEM((parts,) + s.shape, BF16) for s in shards]
    scratch = whole + [
        pltpu.VMEM((parts,) + bias.shape, BF16),
        pltpu.VMEM((SEQ, width), BF16),
        pltpu.VMEM((parts, SEQ, wide), BF16),
        pltpu.VMEM((SEQ, SEQ), F32),
        pltpu.VMEM((parts * heads, 8, SEQ), F32),
        pltpu.VMEM((parts, SEQ, v_wide), BF16),
        pltpu.VMEM((SEQ, width), F32),
        pltpu.VMEM((SEQ, width), BF16),
        pltpu.VMEM((parts, SEQ, hid), BF16),
        pltpu.VMEM((parts, SEQ, hid), BF16),
        pltpu.VMEM((width, SEQ), BF16),
        pltpu.VMEM((SEQ, width), F32),
        pltpu.VMEM((SEQ, 256), F32),
        pltpu.VMEM((SEQ, width), BF16),
        pltpu.VMEM((parts, SEQ, v_wide), BF16),
        pltpu.VMEM((parts, 2, 2, 2, blk, hid), BF16),
        pltpu.VMEM((parts, 2, 2, 2, blk, v_wide), BF16),
        pltpu.VMEM((SEQ, 8), F32),
        pltpu.VMEM((rounds + 1, lines, width), F32),
        pltpu.VMEM((rounds, lines, width), F32),
        pltpu.VMEM((rounds + 1, late_lines, width), F32),
        pltpu.VMEM((rounds, late_lines, width), F32),
    ]
    sizes = [(parts, hid // 2)] * 4 + [(parts, v_wide)] + [(1, wide)] * parts
    for many, n in sizes:
        for lead, half in (((many, 2, 2), 1), ((many, 2), 2), ((many,), 2), ((many, 2), 2), ((many,), 2)):
            scratch.append(pltpu.VMEM(lead + (blk // half, n), BF16))
    for _, n in sizes[: UNITS + 1]:
        scratch.append(pltpu.VMEM((parts - 1, blk, n), BF16))
    scratch += [
        pltpu.SemaphoreType.DMA((5,)),
        pltpu.SemaphoreType.DMA((copies,)),
        pltpu.SemaphoreType.DMA((copies,)),
    ]
    shape = jax.ShapeDtypeStruct
    return pl.pallas_call(
        partial(layer_kernel, dp_size, parts, heads),
        out_shape=[shape(tokens.shape, BF16), shape(tokens.shape, BF16)]
        + [shape(g, F32) for g in grads]
        + [shape((lines, width), F32), shape((late_lines, width), F32), shape(tokens.shape, F32)],
        in_specs=[VMEM] * 4 + [ANY] * 5,
        out_specs=[VMEM] * 9,
        scratch_shapes=scratch,
        compiler_params=pltpu.CompilerParams(
            collective_id=0, has_side_effects=True, vmem_limit_bytes=67043328
        ),
    )(tokens, cot, segments, vecs, bias, *shards)


def regroup(columns, heads):
    lead = columns.shape[:-1]
    split = columns.reshape(lead + (heads, 3, HD))
    pairs = split[..., :2, :].reshape(lead + (heads * 2 * HD,))
    values = split[..., 2, :].reshape(lead + (heads * HD,))
    pad = jnp.zeros(lead + (heads % 2 * HD,), columns.dtype)
    return jnp.concatenate([pairs, values, pad], axis=-1)


def ungroup(columns, heads):
    lead = columns.shape[:-1]
    pairs = columns[..., : heads * 2 * HD].reshape(lead + (heads, 2, HD))
    values = columns[..., heads * 2 * HD : heads * 3 * HD].reshape(lead + (heads, 1, HD))
    return jnp.concatenate([pairs, values], axis=-2)


def on_device(dp_size, parts, tokens, segments, cotangent, ln1_gain, ln1_bias, w_qkv, q_bias, v_bias, w_out, out_bias, ln2_gain, ln2_bias, w_fc1, fc1_bias, w_fc2, fc2_bias):
    tensor_index = lax.axis_index("tensor")
    rows, width = tokens.shape
    head_cols = w_out.shape[0]
    heads = head_cols // HD
    hidden_cols = w_fc1.shape[1]
    vecs = jnp.concatenate([ln1_gain, ln1_bias, out_bias, ln2_gain, ln2_bias, fc2_bias, fc2_bias, fc2_bias])
    vecs = vecs.reshape(8, width).astype(F32)
    out_rows = -(-head_cols // 128) * 128
    out_padded = jnp.pad(w_out, ((0, out_rows - head_cols), (0, 0)))
    qkv = regroup(w_qkv, heads)
    line = max(qkv.shape[1], hidden_cols)
    none = jnp.zeros((16 * line,), BF16)
    pieces = []
    for h in range(heads):
        pieces += [q_bias[h * HD : (h + 1) * HD], none[:HD]]
    pieces += [v_bias, none[: line - 3 * head_cols], fc1_bias, none[: 15 * line - hidden_cols]]
    bias = jnp.concatenate(pieces).reshape(16, line)

    output, grad_tokens, sum_qkv, sum_out, sum_fc1, sum_fc2, small, late, cls_features = layer(
        tokens, cotangent, segments.reshape(-1, SEQ), vecs, bias, [qkv, out_padded, w_fc1, w_fc2], dp_size, parts, heads
    )
    sum_qkv = ungroup(sum_qkv, heads).reshape(sum_qkv.shape[0], -1)
    sum_out = sum_out[:, :head_cols]
    low = dp_size // FAN

    def finish(array):
        if low == 1:
            return array
        groups = [[i * low + j for j in range(low)] for i in range(FAN)]
        return lax.psum_scatter(array, "dp", scatter_dimension=0, axis_index_groups=groups, tiled=True)

    sum_qkv, sum_out, sum_fc1, sum_fc2 = (finish(a) for a in (sum_qkv, sum_out, sum_fc1, sum_fc2))
    mixed_sums = ungroup(late[2 : 2 + parts, : qkv.shape[1]], heads)
    return (
        output,
        grad_tokens,
        cls_features,
        sum_qkv,
        mixed_sums[:, :, 0].reshape(-1),
        mixed_sums[:, :, 2].reshape(-1),
        sum_out.T,
        small[0],
        sum_fc1,
        small[8 : 8 + parts, :hidden_cols].reshape(-1),
        sum_fc2.T,
        small[1],
        late[0],
        late[1],
        small[2],
        small[3],
    )


def solution(mesh):
    dp_size, parts = mesh.shape["dp"], mesh.shape["tensor"]
    row, whole, cols, out_cols = P(("dp", "tensor"), None), P(), P(None, "tensor"), P("tensor")
    down = P("tensor", None)
    in_specs = (row, P("dp"), row, whole, whole, cols, out_cols, out_cols, down, whole, whole, whole, cols, out_cols, down, whole)
    spread, turned = P("dp", "tensor"), P("tensor", "dp")
    out_specs = (row, row, row, spread, whole, whole, turned, whole, spread, whole, turned, whole, whole, whole, whole, whole)
    return jax.shard_map(partial(on_device, dp_size, parts), mesh=mesh, in_specs=in_specs, out_specs=out_specs, check_vma=False)
```

```python
from functools import partial
import math

import jax
import jax.numpy as jnp
import numpy as np
from jax import lax
from jax.experimental import pallas as pl
from jax.experimental.pallas import tpu as pltpu
from jax.sharding import PartitionSpec as P

HD = 64
SEQ = 512
FAN = 8
F32 = jnp.float32
BF16 = jnp.bfloat16
MESH = pl.DeviceIdType.MESH
ANY = pl.BlockSpec(memory_space=pl.ANY)
VMEM = pl.BlockSpec(memory_space=pltpu.VMEM)


def mm(a, b):
    return lax.dot_general(a, b, (((1,), (0,)), ((), ())), preferred_element_type=F32)


def mm_nt(a, b):
    return lax.dot_general(a, b, (((1,), (1,)), ((), ())), preferred_element_type=F32)


def mm_tn(a, b):
    return lax.dot_general(a, b, (((0,), (0,)), ((), ())), preferred_element_type=F32)


class Place:
    def __init__(self, dp_size, parts):
        self.d = lax.axis_index("dp")
        self.t = lax.axis_index("tensor")
        self.dp_size, self.parts = dp_size, parts
        self.low = dp_size // FAN
        block = self.d // self.low
        self.y, self.x, self.c = block // 4, (block // 2) % 2, block % 2

    def flip(self, name):
        stride = self.low * {"y": 4, "x": 2, "c": 1}[name]
        bit = {"y": self.y, "x": self.x, "c": self.c}[name]
        return (self.d + stride * (1 - 2 * bit), self.t)

    def flip_stride(self, stride):
        bit = (self.d // stride) % 2
        return (self.d + stride * (1 - 2 * bit), self.t)

    def shift(self, k):
        return (self.d, (self.t + k) % self.parts)


def greet(partners):
    barrier = pltpu.get_barrier_semaphore()
    for partner in partners:
        pl.semaphore_signal(barrier, inc=1, device_id=partner, device_id_type=MESH)
    pl.semaphore_wait(barrier, len(partners))


class Link:
    def __init__(self, send_sem, recv_sem):
        self.send_sem, self.recv_sem, self.used = send_sem, recv_sem, 0

    def copy(self, src, dst, device):
        made = pltpu.make_async_remote_copy(
            src_ref=src,
            dst_ref=dst,
            send_sem=self.send_sem.at[self.used],
            recv_sem=self.recv_sem.at[self.used],
            device_id=device,
            device_id_type=MESH,
        )
        self.used += 1
        return made


def start(copies):
    for made in copies:
        made.start()


def arrive(copies):
    for made in copies:
        made.wait_recv()


def left(copies):
    for made in copies:
        made.wait_send()


def loop(count, body, hooks=None):
    def step(i, carry):
        for at, hook in (hooks or {}).items():
            pl.when(i == at)(hook)
        body(i)
        return carry

    lax.fori_loop(0, count, step, 0)


def add_into(target, other, lead):
    shape = other.shape[:lead]

    def body(i):
        index = []
        for extent in reversed(shape):
            index.append(i % extent)
            i = i // extent
        index = tuple(reversed(index))
        target_i, other_i = target.at[index], other.at[index]
        target_i[...] = (target_i[...].astype(F32) + other_i[...].astype(F32)).astype(target.dtype)

    loop(math.prod(shape), body)


def gather_unit(here, link, shard, whole):
    parts = here.parts
    y, x, c = here.y, here.x, here.c
    away = pl.ds(1, parts - 1)
    half = whole.shape[4] // 2
    lo, hi = pl.ds(0, half), pl.ds(half, half)
    along = [
        link.copy(shard.at[y, x, c], whole.at[parts - k, y, x, c], here.shift(k))
        for k in range(1, parts)
    ]
    a, b = whole.at[away, y, x, c, lo], whole.at[away, y, x, c, hi]
    first = [link.copy(a, a, here.flip("x")), link.copy(b, b, here.flip("y"))]
    a, b = whole.at[away, y, :, c, lo], whole.at[away, :, x, c, hi]
    second = [link.copy(a, a, here.flip("y")), link.copy(b, b, here.flip("x"))]
    a = whole.at[away, :, :, c]
    third = [link.copy(a, a, here.flip("c"))]
    relay = None
    if parts == 4:
        over = whole.at[2, y, x, c]
        relay = [
            link.copy(over, whole.at[1, y, x, c], here.shift(1)),
            link.copy(over, whole.at[3, y, x, c], here.shift(3)),
        ]
    return Gather(here, along, relay, [first, second, third])


class Gather:
    def __init__(self, here, along, relay, later):
        self.t, self.along, self.relay, self.later = here.t, along, relay, later

    def guarded(self, what, does):
        if self.relay is None:
            for made in self.along:
                does(made)
            return
        up, across, down = self.along[:3]
        ends = (self.t < 3, self.t > 0) if what == "out" else (self.t > 0, self.t < 3)
        pl.when(ends[0])(lambda: does(up))
        does(across)
        pl.when(ends[1])(lambda: does(down))
        for made in self.along[3:]:
            does(made)

    def relayed(self, what, does):
        up, down = self.relay
        at = (2, 1) if what == "out" else (3, 0)
        pl.when(self.t == at[0])(lambda: does(up))
        pl.when(self.t == at[1])(lambda: does(down))

    def begin(self):
        self.guarded("out", lambda made: made.start())

    def step(self, s):
        if s == "z":
            self.guarded("in", lambda made: made.wait_recv())
            if self.relay is not None:
                self.relayed("out", lambda made: made.start())
            return
        if s == 0:
            if self.relay is not None:
                self.relayed("in", lambda made: made.wait_recv())
        else:
            arrive(self.later[s - 1])
        if s < 3:
            start(self.later[s])

    def drain(self):
        self.guarded("out", lambda made: made.wait_send())
        if self.relay is not None:
            self.relayed("out", lambda made: made.wait_send())
        for copies in self.later:
            left(copies)


class Reduction:
    def __init__(self, here, link, grad, first, many, got, got_z):
        self.here, self.got = here, got
        got_c, got_y1, got_x2, got_x1, got_y2 = got
        y, x, c = here.y, here.x, here.c
        half = grad.shape[4] // 2
        self.lo, self.hi = lo, hi = pl.ds(0, half), pl.ds(half, half)
        self.grad = g = grad.at[pl.ds(first, many)]
        self.stages = [
            [link.copy(g.at[:, :, :, 1 - c], got_c, here.flip("c"))],
            [
                link.copy(g.at[:, 1 - y, :, c, lo], got_y1, here.flip("y")),
                link.copy(g.at[:, :, 1 - x, c, hi], got_x1, here.flip("x")),
            ],
            [
                link.copy(g.at[:, y, 1 - x, c, lo], got_x2, here.flip("x")),
                link.copy(g.at[:, 1 - y, x, c, hi], got_y2, here.flip("y")),
            ],
            [
                link.copy(grad.at[k, y, x, c], got_z.at[k - 1], here.shift(k))
                for k in range(first, first + many)
                if k > 0
            ],
        ]

    def step(self, s):
        y, x, c = self.here.y, self.here.x, self.here.c
        g, lo, hi = self.grad, self.lo, self.hi
        got_c, got_y1, got_x2, got_x1, got_y2 = self.got
        if s > 0:
            arrive(self.stages[s - 1])
        if s == 1:
            add_into(g.at[:, :, :, c], got_c, 3)
        if s == 2:
            add_into(g.at[:, y, :, c, lo], got_y1, 2)
            add_into(g.at[:, :, x, c, hi], got_x1, 2)
        if s == 3:
            add_into(g.at[:, y, x, c, lo], got_x2, 1)
            add_into(g.at[:, y, x, c, hi], got_y2, 1)
        if s < 4:
            start(self.stages[s])

    def drain(self):
        for copies in self.stages:
            left(copies)


def normalize(values):
    average = jnp.mean(values, axis=-1, keepdims=True)
    centered = values - average
    spread = jnp.mean(centered * centered, axis=-1, keepdims=True)
    scale = lax.rsqrt(spread + 1e-06)
    return centered * scale, scale


def normalize_back(hat, scale, gain, grad):
    scaled = grad * gain
    return (
        scaled
        - jnp.mean(scaled, axis=-1, keepdims=True)
        - hat * jnp.mean(scaled * hat, axis=-1, keepdims=True)
    ) * scale


ROWS = 64
UNITS = 5
NAMES = (
    "tokens",
    "cot",
    "segments",
    "vecs",
    "bias",
    "w_qkv",
    "w_out",
    "w_fc1",
    "w_fc2",
)
OUTS = (
    "output",
    "g_tokens",
    "s_qkv",
    "s_out",
    "s_fc1",
    "s_fc2",
    "small",
    "cls",
)
SCRATCH = (
    "f_qkv",
    "f_out",
    "f_fc1",
    "f_fc2",
    "biases",
    "normed",
    "mixed",
    "mask",
    "lse",
    "heads",
    "resid",
    "normed2",
    "active",
    "slope",
    "turned",
    "acc",
    "g_low",
    "g_heads",
    "g_fc2",
    "g_out",
    "cols",
    "sums",
    "got_small",
    "all_sums",
)


def layer_kernel(dp_size, parts, heads, *refs):
    refs = list(refs)
    ref = {}
    for name in NAMES + OUTS + SCRATCH:
        ref[name] = refs.pop(0)
    got = [[refs.pop(0) for _ in range(5)] for _ in range(UNITS + parts)]
    got_z = [refs.pop(0) for _ in range(UNITS + 1)]
    local_sem, send_sem, recv_sem = refs
    tokens, cot, cols, vecs = ref["tokens"], ref["cot"], ref["cols"], ref["vecs"]
    segments = ref["segments"]
    f_qkv, f_out, f_fc1, f_fc2 = ref["f_qkv"], ref["f_out"], ref["f_fc1"], ref["f_fc2"]
    biases, normed, mixed, mask = ref["biases"], ref["normed"], ref["mixed"], ref["mask"]
    lse, hd, resid, normed2 = ref["lse"], ref["heads"], ref["resid"], ref["normed2"]
    active, slope, turned, acc = ref["active"], ref["slope"], ref["turned"], ref["acc"]
    tile = acc.at[:, pl.ds(0, 256)]
    g_low, g_heads, sums = ref["g_low"], ref["g_heads"], ref["sums"]
    g_fc2, g_out = ref["g_fc2"], ref["g_out"]
    g_mixed = active
    wide = f_qkv.shape[5]
    g_qkv = f_fc1.at[:, :, :, :, :, pl.ds(0, wide)]
    g_fc1 = f_fc2
    width = tokens.shape[1]
    small = sums.at[0]
    here = Place(dp_size, parts)
    qk_wide = heads * 128
    strides = [1 << b for b in range(dp_size.bit_length() - 1)]
    bits = [here.flip_stride(s) for s in strides]
    link = Link(send_sem, recv_sem)

    shards = [ref[n] for n in ("w_qkv", "w_out", "w_fc1", "w_fc2")]
    wholes = [f_qkv, f_out, f_fc1, f_fc2]
    own = [
        pltpu.make_async_copy(a, b.at[0], local_sem.at[i])
        for i, (a, b) in enumerate(zip(shards + [ref["bias"]], wholes + [biases]))
    ]
    start(own)
    greet(bits + [here.shift(k) for k in range(1, parts)])
    def columns(array, first, many):
        return array.at[:, :, :, :, pl.ds(first, many)] if len(array.shape) == 5 else array.at[:, :, :, :, :, pl.ds(first, many)]

    cut = f_fc1.shape[5] // 2
    plans = {"q": gather_unit(here, link, shards[0], f_qkv), "o": gather_unit(here, link, shards[1], f_out)}
    for name, i, first in (("a", 2, 0), ("b", 2, cut), ("c", 3, 0), ("d", 3, cut)):
        plans[name] = gather_unit(
            here, link, columns(shards[i], first, cut), columns(wholes[i], first, cut)
        )
    plans["q"].along += [
        link.copy(ref["bias"], biases.at[parts - k], here.shift(k)) for k in range(1, parts)
    ]
    for name in "qoa":
        plans[name].begin()
    units = {}
    for i, (name, grad) in enumerate(
        (
            ("A", columns(g_fc2, 0, cut)),
            ("B", columns(g_fc2, cut, cut)),
            ("C", columns(g_fc1, 0, cut)),
            ("D", columns(g_fc1, cut, cut)),
            ("O", g_out),
        )
    ):
        units[name] = Reduction(here, link, grad, 0, parts, got[i], got_z[i])
    for k in range(parts):
        units[k] = Reduction(here, link, g_qkv, k, 1, got[UNITS + k], got_z[UNITS])

    def fwd(*steps):
        def run():
            for name, s in steps:
                if s == "go":
                    plans[name].begin()
                else:
                    plans[name].step(s)

        return run

    def red(*steps):
        def run():
            for name, s in steps:
                units[name].step(s)

        return run

    def total(grad, got_last, out=None):
        value = grad[0, here.y, here.x, here.c].astype(F32)
        for k in range(parts - 1):
            value += got_last[k].astype(F32)
        if out is None:
            return value
        out[...] = value

    trips = [
        link.copy(sums.at[r], ref["got_small"].at[r], partner) for r, partner in enumerate(bits)
    ]
    all_sums = ref["all_sums"]
    spread_out = [
        link.copy(sums.at[len(bits)], all_sums.at[here.t], here.shift(k)) for k in range(1, parts)
    ]

    def small_round(r):
        if r > 0:
            arrive([trips[r - 1]])
            sums[r] = sums[r - 1] + ref["got_small"][r - 1]
        if r < len(trips):
            start([trips[r]])
        else:
            start(spread_out)
            all_sums[here.t] = sums[r]

    def gain(i):
        return vecs[pl.ds(i, 1), :].astype(F32)

    chunks = SEQ // ROWS

    def rows_of(i):
        return pl.ds(pl.multiple_of(i * ROWS, ROWS), ROWS)

    small[...] = jnp.zeros_like(small)
    labels = jnp.concatenate(
        [segments[pl.ds(here.t * (SEQ // 128) + i, 1), :] for i in range(SEQ // 128)], axis=1
    )
    spot = lax.broadcasted_iota(jnp.int32, (1, SEQ), 1)
    earlier = pltpu.roll(labels, 1, 1)
    begins = (labels >= 0) & ((spot == 0) | (labels != earlier))
    line = labels.astype(F32)
    kinds = lax.broadcasted_iota(jnp.int32, (8, SEQ), 0)
    stacked = jnp.where(kinds == 0, line, jnp.where(kinds == 1, (labels >= 0).astype(F32), begins.astype(F32)))
    cols[...] = stacked.T

    def norm_one(i):
        r = rows_of(i)
        hat, _ = normalize(tokens[r, :].astype(F32))
        normed[r, :] = (hat * gain(0) + gain(1)).astype(BF16)
        mask[r, :] = jnp.where(cols[r, 0:1] == line, 0.0, -1e30)

    loop(chunks, norm_one)

    low_half = lax.broadcasted_iota(jnp.int32, (SEQ, 128), 1) < 64

    head_cols = heads * HD
    pick = active.at[0, pl.ds(0, 2 * head_cols), pl.ds(0, wide)]
    taken = lax.broadcasted_iota(jnp.int32, (2 * head_cols, wide), 0)
    slot = lax.broadcasted_iota(jnp.int32, (2 * head_cols, wide), 1)
    lane = slot % 128
    of_q = (slot < qk_wide) & (lane < HD) & (taken == (slot // 128) * HD + lane)
    of_v = (slot >= qk_wide) & (taken == head_cols + slot - qk_wide)
    pick[...] = jnp.where(of_q | of_v, 1.0, 0.0).astype(BF16)

    def qkv_part(k):
        offset = mm(biases[k, :, pl.ds(0, 2 * head_cols)].astype(BF16), pick[...])[6:7]
        for at in range(0, wide, 256):
            size = min(256, wide - at)
            w = f_qkv[k, :, :, :, :, pl.ds(at, size)].reshape(width, size)
            out = mm(normed[...], w) + offset[:, at : at + size]
            mixed[k, :, pl.ds(at, size)] = out.astype(BF16)

    def head_place(i):
        k, j = i // heads, i % heads
        at = pl.ds(pl.multiple_of(j * 128, 128), 128)
        v_at = pl.ds(pl.multiple_of(qk_wide + (j // 2) * 128, 128), 128)
        h_at = pl.ds(pl.multiple_of((j // 2) * 128, 128), 128)
        even = j % 2 == 0
        return k, at, v_at, h_at, even

    def scores_of(k, at):
        qk = mixed[k, :, at].astype(F32)
        q = jnp.where(low_half, qk * (1.0 / math.sqrt(HD)), 0.0).astype(BF16)
        kq = pltpu.roll(qk, 64, 1).astype(BF16)
        return mm_nt(kq, q) + mask[...], kq

    def mine_of(even):
        return low_half == even

    def attend(i):
        k, at, v_at, h_at, even = head_place(i)
        scores, _ = scores_of(k, at)
        highest = jnp.max(scores, axis=0, keepdims=True)
        expon = jnp.exp(scores - highest)
        total = jnp.sum(expon, axis=0, keepdims=True)
        lse[i, 0:1, :] = highest + jnp.log(total)
        weights = (expon * (1.0 / total)).astype(BF16)
        out = mm_tn(weights, mixed[k, :, v_at])
        before = jnp.where(even, 0.0, hd[k, :, h_at].astype(F32))
        hd[k, :, h_at] = jnp.where(mine_of(even), out, before).astype(BF16)

    own[0].wait()
    own[4].wait()
    qkv_part(0)
    loop(heads, attend, {1: fwd(("q", "z"))})
    fwd(("o", "z"), ("b", "go"), ("q", 0), ("o", 0))()
    fwd(("a", "z"), ("c", "go"), ("q", 1), ("a", 0), ("o", 1), ("b", "z"), ("d", "go"), ("q", 2))()
    fwd(("b", 0), ("a", 1), ("c", "z"), ("q", 3))()
    loop(parts - 1, lambda k: qkv_part(k + 1))
    loop(
        heads * (parts - 1),
        lambda i: attend(i + heads),
        {
            1: fwd(("o", 2), ("c", 0), ("d", "z")),
            2: fwd(("b", 1), ("d", 0)),
            3: fwd(("a", 2)),
            4: fwd(("o", 3)),
            5: fwd(("c", 1)),
            6: fwd(("b", 2), ("a", 3)),
            7: fwd(("d", 1)),
            8: fwd(("c", 2)),
        },
    )
    for made in own[1:4]:
        made.wait()

    def project(n):
        at = pl.ds(pl.multiple_of(n * 256, 256), 256)
        total = tokens[:, at].astype(F32) + vecs[2:3, at].astype(F32)
        for k in range(parts):
            total += mm(hd[k], f_out[k, :, :, :, :, at].reshape(-1, 256))
        resid[:, at] = total

    loop(width // 256, project)

    def norm_two(i):
        r = rows_of(i)
        hat, _ = normalize(resid[r, :])
        normed2[r, :] = (hat * gain(3) + gain(4)).astype(BF16)

    loop(chunks, norm_two)
    hid = f_fc1.shape[5]
    tiles = hid // 256

    def fc1_tile(i):
        k, n = i // tiles, i % tiles
        at = pl.ds(pl.multiple_of(n * 256, 256), 256)
        tile[...] = mm(normed2[...], f_fc1[k, :, :, :, :, at].reshape(width, 256)) + biases[
            k, 7:8, at
        ].astype(F32)

        def gelu(j):
            r = rows_of(j)
            v = tile[r, :]
            cdf = 0.5 * (1.0 + lax.erf(v * (1.0 / math.sqrt(2.0))))
            pdf = jnp.exp(-0.5 * v * v) * (1.0 / math.sqrt(2.0 * math.pi))
            active[k, r, at] = (v * cdf).astype(BF16)
            slope[k, r, at] = (cdf + v * pdf).astype(BF16)

        loop(chunks, gelu)

    loop(tiles, fc1_tile)
    fwd(("b", 3))()
    loop(
        tiles * (parts - 1),
        lambda i: fc1_tile(i + tiles),
        {2: fwd(("d", 2)), 4: fwd(("c", 3))},
    )

    def grad_branch(i):
        r = rows_of(i)
        g_low[r, :] = (cot[r, :].astype(F32) * cols[r, 1:2]).astype(BF16)

    loop(chunks, grad_branch)
    ones = jnp.ones((8, SEQ), BF16)

    def turn(source):
        def body(n):
            at = pl.ds(pl.multiple_of(n * 256, 256), 256)
            turned[at, :] = source[:, at].astype(F32).T.astype(BF16)

        loop(width // 256, body)

    def weight_grad(target, source, columns, parts_here=parts):
        def body(k):
            for at in range(0, columns, 256):
                size = min(256, columns - at)
                out = mm(turned[...], source[k, :, pl.ds(at, size)])
                target[k, :, :, :, :, pl.ds(at, size)] = out.astype(BF16).reshape(
                    2, 2, 2, width // FAN, size
                )

        return body

    turn(g_low)
    small[1:2, :] = mm(ones, g_low[...])[0:1]
    loop(parts, weight_grad(g_fc2, active, hid))
    red(("A", 0), ("B", 0))()
    fwd(("d", 3))()
    for plan in plans.values():
        plan.drain()

    def finish(n):
        at = pl.ds(pl.multiple_of(n * 256, 256), 256)
        total = resid[:, at] + vecs[5:6, at].astype(F32)
        for k in range(parts):
            total += mm(active[k], f_fc2[k, :, :, :, :, at].reshape(hid, 256))
        out = total.astype(BF16)
        ref["output"][:, at] = out
        values = out.astype(F32)
        picked = values * cols[:, 2:3]
        small[4:5, at] = jnp.sum(picked, axis=0, keepdims=True)
        small[5:6, at] = jnp.sum(picked * values, axis=0, keepdims=True)

    loop(width // 256, finish, {2: red(("A", 1))})
    red(("B", 1))()
    small[6:7, :] = jnp.broadcast_to(jnp.sum(cols[:, 2:3], axis=0, keepdims=True), (1, width))
    side = hid // 2

    def hidden_back(i):
        k, s = i // 2, i % 2
        at = pl.ds(pl.multiple_of(s * side, 128), side)
        back = mm_nt(g_low[...], f_fc2[k, s].reshape(side, width))
        back = (back * slope[k, :, at].astype(F32)).astype(BF16)
        slope[k, :, at] = back
        row = pl.ds(10 + (here.t + k) % parts, 1)
        small[row, at] = mm(ones, back)[0:1]

    loop(2 * parts, hidden_back, {6: red(("A", 2))})
    turn(normed2)
    loop(parts, weight_grad(g_fc1, slope, hid))
    red(("C", 0), ("D", 0), ("B", 2))()

    def normed2_back(s):
        at = pl.ds(pl.multiple_of(s * side, 128), side)
        total = mm_nt(slope[0], f_fc1[0, s].reshape(side, hid))
        for k in range(1, parts):
            total += mm_nt(slope[k], f_fc1[k, s].reshape(side, hid))
        acc[:, at] = total

    loop(2, normed2_back, {1: red(("C", 1))})
    red(("D", 1), ("A", 3))()

    def norm_two_back(i):
        r = rows_of(i)
        grad = acc[r, :]
        hat, scale = normalize(resid[r, :])
        back = cot[r, :].astype(F32) * cols[r, 1:2] + normalize_back(hat, scale, gain(3), grad)
        acc[r, :] = back
        g_low[r, :] = back.astype(BF16)
        small[2:3, :] += jnp.sum(grad * hat, axis=0, keepdims=True)
        small[3:4, :] += jnp.sum(grad, axis=0, keepdims=True)
        small[0:1, :] += jnp.sum(back, axis=0, keepdims=True)

    loop(chunks, norm_two_back)
    turn(g_low)
    v_wide = hd.shape[2]
    loop(parts, weight_grad(g_out, hd, v_wide))
    red(("O", 0), ("B", 3))()

    def heads_back(k):
        g_heads[k] = mm_nt(g_low[...], f_out[k].reshape(v_wide, width)).astype(BF16)

    loop(parts, heads_back)

    def attend_back(i):
        k, at, v_at, h_at, even = head_place(i)
        mine = mine_of(even)
        scores, kq = scores_of(k, at)
        weights = jnp.exp(scores - lse[i, 0:1, :])
        grad = g_heads[k, :, h_at]
        own_grad = jnp.where(mine, grad.astype(F32), 0.0).astype(BF16)
        g_value = mm(weights.astype(BF16), grad)
        g_weights = mm_nt(mixed[k, :, v_at], own_grad)
        inner = jnp.sum(g_weights * weights, axis=0, keepdims=True)
        g_scores = (weights * (g_weights - inner)).astype(BF16)
        g_q = mm_tn(g_scores, kq)
        g_k = mm(g_scores, kq)
        both = jnp.where(low_half, g_q, g_k) * (1.0 / math.sqrt(HD))
        g_mixed[k, :, at] = both.astype(BF16)
        before = jnp.where(even, 0.0, g_mixed[k, :, v_at].astype(F32))
        g_mixed[k, :, v_at] = jnp.where(mine, g_value, before).astype(BF16)

    turn(normed)

    def qkv_grad(k):
        def run():
            weight_grad(g_qkv, g_mixed, wide)(k)
            units[k].step(0)
            row = pl.ds(10 + parts + (here.t + k) % parts, 1)
            small[row, pl.ds(0, wide)] = mm(ones, g_mixed[k, :, pl.ds(0, wide)])[0:1]

        return run

    hooks = {}

    def hook(at, *runs):
        hooks.setdefault(at, []).extend(runs)

    for k in range(1, parts):
        hook(heads * k, qkv_grad(k - 1))
    hook(1, red(("C", 2)))
    hook(2, red(("O", 1)))
    hook(5, red(("D", 2)))
    hook(7, red((0, 1)))
    hook(8, red(("A", 4), ("C", 3)))
    hook(9, red((1, 1)))
    hook(10, red(("O", 2)))
    hook(11, red(("D", 3), (0, 2)))

    def joined(runs):
        def run():
            for one in runs:
                one()

        return run

    loop(heads * parts, attend_back, {at: joined(runs) for at, runs in hooks.items()})
    qkv_grad(parts - 1)()
    for k in range(2, parts - 1):
        red((k, 1))()

    def normed_back(s):
        at = pl.ds(pl.multiple_of(s * side, 128), side)
        total = mm_nt(g_mixed[0, :, pl.ds(0, wide)], f_qkv[0, s].reshape(side, wide))
        for k in range(1, parts):
            total += mm_nt(g_mixed[k, :, pl.ds(0, wide)], f_qkv[k, s].reshape(side, wide))
        tile_out = total
        resid[:, at] = tile_out

    loop(2, normed_back, {1: red((parts - 1, 1), (1, 2), ("O", 3))})

    def norm_one_back(i):
        r = rows_of(i)
        grad = resid[r, :]
        hat, scale = normalize(tokens[r, :].astype(F32))
        back = acc[r, :] + normalize_back(hat, scale, gain(0), grad)
        ref["g_tokens"][r, :] = back.astype(BF16)
        small[8:9, :] += jnp.sum(grad * hat, axis=0, keepdims=True)
        small[9:10, :] += jnp.sum(grad, axis=0, keepdims=True)

    loop(chunks, norm_one_back)
    small_round(0)
    for k in range(2, parts):
        red((k, 2))()
    red(("B", 4), ("C", 4), ("D", 4), ("O", 4))()
    small_round(1)
    total(columns(g_fc1, 0, cut), got_z[2], ref["s_fc1"].at[:, pl.ds(0, cut)])
    total(columns(g_fc1, cut, cut), got_z[3], ref["s_fc1"].at[:, pl.ds(cut, cut)])
    for k in range(parts):
        red((k, 3))()
    small_round(2)
    total(g_out, got_z[4], ref["s_out"])
    for r in range(3, len(trips) + 1):
        small_round(r)
    for i, first in enumerate((0, cut)):
        total(columns(g_fc2, first, cut), got_z[i], ref["s_fc2"].at[:, pl.ds(first, cut)])
    for k in range(parts):
        red((k, 4))()
    triple = 3 * HD
    source = lax.broadcasted_iota(jnp.int32, (wide, heads * triple), 0)
    target = lax.broadcasted_iota(jnp.int32, (wide, heads * triple), 1)
    head, lane = target // triple, target % triple
    wanted = jnp.where(lane < 2 * HD, head * 2 * HD + lane, qk_wide + head * HD + lane - 2 * HD)
    unpick = jnp.where(source == wanted, 1.0, 0.0)
    ref["s_qkv"][...] = lax.dot_general(
        total(g_qkv, got_z[UNITS]),
        unpick,
        (((1,), (0,)), ((), ())),
        precision=lax.Precision.HIGHEST,
        preferred_element_type=F32,
    )
    arrive(spread_out)
    final = all_sums[0]
    for t in range(1, parts):
        final += all_sums[t]
    ref["small"][...] = final
    source = lax.broadcasted_iota(jnp.int32, (wide, 2 * head_cols), 0)
    target = lax.broadcasted_iota(jnp.int32, (wide, 2 * head_cols), 1)
    wanted = jnp.where(
        target < head_cols, (target // HD) * 2 * HD + target % HD, qk_wide + target - head_cols
    )
    ref["small"][pl.ds(10 + parts, parts), pl.ds(0, 2 * head_cols)] = lax.dot_general(
        final[:, :wide],
        jnp.where(source == wanted, 1.0, 0.0),
        (((1,), (0,)), ((), ())),
        precision=lax.Precision.HIGHEST,
        preferred_element_type=F32,
    )[10 + parts : 10 + 2 * parts]
    mean = final[4:5, :] / final[6:7, :]
    spread = final[5:6, :] / final[6:7, :] - mean * mean
    spread = lax.rsqrt(spread + 1e-05)

    def features(i):
        r = rows_of(i)
        ref["cls"][r, :] = cols[r, 2:3] * (ref["output"][r, :].astype(F32) - mean) * spread

    loop(chunks, features)
    left(trips + spread_out)
    for unit in units.values():
        unit.drain()


def layer(tokens, cot, segments, bias, shards, dp_size, parts, heads):
    shards = [s.reshape(2, 2, 2, s.shape[0] // FAN, s.shape[1]) for s in shards]
    width, hid = tokens.shape[1], shards[2].shape[4]
    wide, v_wide = shards[0].shape[4], FAN * shards[1].shape[3]
    lines = -(-(10 + 2 * parts) // 8) * 8
    rounds = dp_size.bit_length() - 1
    copies = 6 * (5 + parts + 1) + parts - 1 + (UNITS + parts) * (5 + parts) + rounds + parts
    blk = width // FAN
    grads = [(blk, wide), (blk, v_wide), (blk, hid), (blk, hid)]
    whole = [pltpu.VMEM((parts,) + s.shape, BF16) for s in shards]
    scratch = whole + [
        pltpu.VMEM((parts,) + bias.shape, F32),
        pltpu.VMEM((SEQ, width), BF16),
        pltpu.VMEM((parts, SEQ, wide), BF16),
        pltpu.VMEM((SEQ, SEQ), F32),
        pltpu.VMEM((parts * heads, 8, SEQ), F32),
        pltpu.VMEM((parts, SEQ, v_wide), BF16),
        pltpu.VMEM((SEQ, width), F32),
        pltpu.VMEM((SEQ, width), BF16),
        pltpu.VMEM((parts, SEQ, hid), BF16),
        pltpu.VMEM((parts, SEQ, hid), BF16),
        pltpu.VMEM((width, SEQ), BF16),
        pltpu.VMEM((SEQ, width), F32),
        pltpu.VMEM((SEQ, width), BF16),
        pltpu.VMEM((parts, SEQ, v_wide), BF16),
        pltpu.VMEM((parts, 2, 2, 2, blk, hid), BF16),
        pltpu.VMEM((parts, 2, 2, 2, blk, v_wide), BF16),
        pltpu.VMEM((SEQ, 8), F32),
        pltpu.VMEM((rounds + 1, lines, width), F32),
        pltpu.VMEM((rounds, lines, width), F32),
        pltpu.VMEM((parts, lines, width), F32),
    ]
    sizes = [(parts, hid // 2)] * 4 + [(parts, v_wide)] + [(1, wide)] * parts
    for many, n in sizes:
        for lead, half in (((many, 2, 2), 1), ((many, 2), 2), ((many,), 2), ((many, 2), 2), ((many,), 2)):
            scratch.append(pltpu.VMEM(lead + (blk // half, n), BF16))
    for _, n in sizes[: UNITS + 1]:
        scratch.append(pltpu.VMEM((parts - 1, blk, n), BF16))
    scratch += [
        pltpu.SemaphoreType.DMA((5,)),
        pltpu.SemaphoreType.DMA((copies,)),
        pltpu.SemaphoreType.DMA((copies,)),
    ]
    shape = jax.ShapeDtypeStruct
    return pl.pallas_call(
        partial(layer_kernel, dp_size, parts, heads),
        out_shape=[shape(tokens.shape, BF16), shape(tokens.shape, BF16)]
        + [shape((blk, heads * 3 * HD), F32), shape((blk, v_wide), F32), shape((blk, hid), F32), shape((blk, hid), F32)]
        + [shape((lines, width), F32), shape(tokens.shape, F32)],
        in_specs=[VMEM] * 4 + [ANY] * 5,
        out_specs=[VMEM] * 8,
        scratch_shapes=scratch,
        compiler_params=pltpu.CompilerParams(
            collective_id=0, has_side_effects=True, vmem_limit_bytes=67043328
        ),
    )(tokens, cot, segments, bias, bias, *shards)


def regroup(columns, heads):
    wide = heads * 2 * HD + -(-heads // 2) * 2 * HD
    wanted = np.arange(heads * 3 * HD).reshape(heads, 3, HD)
    source = np.concatenate([wanted[:, :2].reshape(-1), wanted[:, 2].reshape(-1)])
    pick = np.zeros((heads * 3 * HD, wide), np.float32)
    pick[source, np.arange(source.size)] = 1.0
    return jnp.dot(columns, jnp.asarray(pick, BF16), preferred_element_type=F32).astype(BF16)


def on_device(dp_size, parts, tokens, segments, cotangent, ln1_gain, ln1_bias, w_qkv, q_bias, v_bias, w_out, out_bias, ln2_gain, ln2_bias, w_fc1, fc1_bias, w_fc2, fc2_bias):
    tensor_index = lax.axis_index("tensor")
    rows, width = tokens.shape
    head_cols = w_out.shape[0]
    heads = head_cols // HD
    hidden_cols = w_fc1.shape[1]
    out_rows = -(-head_cols // 128) * 128
    out_padded = jnp.pad(w_out, ((0, out_rows - head_cols), (0, 0)))
    qkv = regroup(w_qkv, heads)
    line = max(2 * head_cols, hidden_cols, width)

    def fit(vector):
        return jnp.pad(vector, (0, line - vector.shape[0]))

    rows = [ln1_gain, ln1_bias, out_bias, ln2_gain, ln2_bias, fc2_bias, jnp.concatenate([q_bias, v_bias]), fc1_bias]
    bias = jnp.stack([fit(row) for row in rows]).astype(F32)

    output, grad_tokens, sum_qkv, sum_out, sum_fc1, sum_fc2, small, cls_features = layer(
        tokens, cotangent, segments.reshape(-1, 128), bias, [qkv, out_padded, w_fc1, w_fc2], dp_size, parts, heads
    )
    low = dp_size // FAN

    def finish(array, axis):
        if low == 1:
            return array
        groups = [[i * low + j for j in range(low)] for i in range(FAN)]
        return lax.psum_scatter(array, "dp", scatter_dimension=axis, axis_index_groups=groups, tiled=True)

    sum_qkv, sum_fc1, sum_out, sum_fc2 = (
        finish(a, 0) for a in (sum_qkv, sum_fc1, sum_out[:, :head_cols], sum_fc2)
    )
    start = 10 + parts
    mixed_sums = small[start : start + parts]
    return (
        output,
        grad_tokens,
        cls_features,
        sum_qkv,
        mixed_sums[:, :head_cols].reshape(-1),
        mixed_sums[:, head_cols : 2 * head_cols].reshape(-1),
        sum_out.T,
        small[0],
        sum_fc1,
        small[10 : 10 + parts, :hidden_cols].reshape(-1),
        sum_fc2.T,
        small[1],
        small[8],
        small[9],
        small[2],
        small[3],
    )


def solution(mesh):
    dp_size, parts = mesh.shape["dp"], mesh.shape["tensor"]
    row, whole, cols, out_cols = P(("dp", "tensor"), None), P(), P(None, "tensor"), P("tensor")
    down = P("tensor", None)
    in_specs = (row, P("dp"), row, whole, whole, cols, out_cols, out_cols, down, whole, whole, whole, cols, out_cols, down, whole)
    spread, turned = P("dp", "tensor"), P("tensor", "dp")
    out_specs = (row, row, row, spread, whole, whole, turned, whole, spread, whole, turned, whole, whole, whole, whole, whole)
    return jax.shard_map(partial(on_device, dp_size, parts), mesh=mesh, in_specs=in_specs, out_specs=out_specs, check_vma=False)
```

```python
from functools import partial
import math

import jax
import jax.numpy as jnp
import numpy as np
from jax import lax
from jax.experimental import pallas as pl
from jax.experimental.pallas import tpu as pltpu
from jax.sharding import PartitionSpec as P

HD = 64
SEQ = 512
FAN = 8
F32 = jnp.float32
BF16 = jnp.bfloat16
MESH = pl.DeviceIdType.MESH
ANY = pl.BlockSpec(memory_space=pl.ANY)
VMEM = pl.BlockSpec(memory_space=pltpu.VMEM)


def mm(a, b):
    return lax.dot_general(a, b, (((1,), (0,)), ((), ())), preferred_element_type=F32)


def mm_nt(a, b):
    return lax.dot_general(a, b, (((1,), (1,)), ((), ())), preferred_element_type=F32)


def mm_tn(a, b):
    return lax.dot_general(a, b, (((0,), (0,)), ((), ())), preferred_element_type=F32)


class Place:
    def __init__(self, dp_size, parts):
        self.d = lax.axis_index("dp")
        self.t = lax.axis_index("tensor")
        self.dp_size, self.parts = dp_size, parts
        self.low = dp_size // FAN
        block = self.d // self.low
        self.y, self.x, self.c = block // 4, (block // 2) % 2, block % 2

    def flip(self, name):
        stride = self.low * {"y": 4, "x": 2, "c": 1}[name]
        bit = {"y": self.y, "x": self.x, "c": self.c}[name]
        return (self.d + stride * (1 - 2 * bit), self.t)

    def flip_stride(self, stride):
        bit = (self.d // stride) % 2
        return (self.d + stride * (1 - 2 * bit), self.t)

    def shift(self, k):
        return (self.d, (self.t + k) % self.parts)


def greet(partners):
    barrier = pltpu.get_barrier_semaphore()
    for partner in partners:
        pl.semaphore_signal(barrier, inc=1, device_id=partner, device_id_type=MESH)
    pl.semaphore_wait(barrier, len(partners))


class Link:
    def __init__(self, send_sem, recv_sem):
        self.send_sem, self.recv_sem, self.used = send_sem, recv_sem, 0

    def copy(self, src, dst, device):
        made = pltpu.make_async_remote_copy(
            src_ref=src,
            dst_ref=dst,
            send_sem=self.send_sem.at[self.used],
            recv_sem=self.recv_sem.at[self.used],
            device_id=device,
            device_id_type=MESH,
        )
        self.used += 1
        return made


def start(copies):
    for made in copies:
        made.start()


def arrive(copies):
    for made in copies:
        made.wait_recv()


def left(copies):
    for made in copies:
        made.wait_send()


def loop(count, body, hooks=None):
    def step(i, carry):
        for at, hook in (hooks or {}).items():
            pl.when(i == at)(hook)
        body(i)
        return carry

    lax.fori_loop(0, count, step, 0)


def add_into(target, other, lead):
    shape = other.shape[:lead]

    def body(i):
        index = []
        for extent in reversed(shape):
            index.append(i % extent)
            i = i // extent
        index = tuple(reversed(index))
        target_i, other_i = target.at[index], other.at[index]
        target_i[...] = (target_i[...].astype(F32) + other_i[...].astype(F32)).astype(target.dtype)

    loop(math.prod(shape), body)


def gather_unit(here, link, shard, whole):
    parts = here.parts
    y, x, c = here.y, here.x, here.c
    away = pl.ds(1, parts - 1)
    half = whole.shape[4] // 2
    lo, hi = pl.ds(0, half), pl.ds(half, half)
    along = [
        link.copy(shard.at[y, x, c], whole.at[parts - k, y, x, c], here.shift(k))
        for k in range(1, parts)
    ]
    a, b = whole.at[away, y, x, c, lo], whole.at[away, y, x, c, hi]
    first = [link.copy(a, a, here.flip("x")), link.copy(b, b, here.flip("y"))]
    a, b = whole.at[away, y, :, c, lo], whole.at[away, :, x, c, hi]
    second = [link.copy(a, a, here.flip("y")), link.copy(b, b, here.flip("x"))]
    a = whole.at[away, :, :, c]
    third = [link.copy(a, a, here.flip("c"))]
    relay = None
    if parts == 4:
        over = whole.at[2, y, x, c]
        relay = [
            link.copy(over, whole.at[1, y, x, c], here.shift(1)),
            link.copy(over, whole.at[3, y, x, c], here.shift(3)),
        ]
    return Gather(here, along, relay, [first, second, third])


class Gather:
    def __init__(self, here, along, relay, later):
        self.t, self.along, self.relay, self.later = here.t, along, relay, later
        self.extra = []

    def guarded(self, what, does):
        if self.relay is None:
            for made in self.along:
                does(made)
            return
        up, across, down = self.along[:3]
        ends = (self.t < 3, self.t > 0) if what == "out" else (self.t > 0, self.t < 3)
        pl.when(ends[0])(lambda: does(up))
        does(across)
        pl.when(ends[1])(lambda: does(down))

    def relayed(self, what, does):
        up, down = self.relay
        at = (2, 1) if what == "out" else (3, 0)
        pl.when(self.t == at[0])(lambda: does(up))
        pl.when(self.t == at[1])(lambda: does(down))

    def begin(self):
        self.guarded("out", lambda made: made.start())

    def step(self, s):
        if s == "z":
            self.guarded("in", lambda made: made.wait_recv())
            arrive(self.extra)
            if self.relay is not None:
                self.relayed("out", lambda made: made.start())
            return
        if s == 0:
            if self.relay is not None:
                self.relayed("in", lambda made: made.wait_recv())
        else:
            arrive(self.later[s - 1])
        if s < 3:
            start(self.later[s])

    def drain(self):
        self.guarded("out", lambda made: made.wait_send())
        if self.relay is not None:
            self.relayed("out", lambda made: made.wait_send())
        for copies in self.later + [self.extra]:
            left(copies)


class Reduction:
    def __init__(self, here, link, grad, first, many, got, got_z):
        self.here, self.got = here, got
        got_c, got_y1, got_x2, got_x1, got_y2 = got
        y, x, c = here.y, here.x, here.c
        half = grad.shape[4] // 2
        self.lo, self.hi = lo, hi = pl.ds(0, half), pl.ds(half, half)
        self.grad = g = grad.at[pl.ds(first, many)]
        self.stages = [
            [link.copy(g.at[:, :, :, 1 - c], got_c, here.flip("c"))],
            [
                link.copy(g.at[:, 1 - y, :, c, lo], got_y1, here.flip("y")),
                link.copy(g.at[:, :, 1 - x, c, hi], got_x1, here.flip("x")),
            ],
            [
                link.copy(g.at[:, y, 1 - x, c, lo], got_x2, here.flip("x")),
                link.copy(g.at[:, 1 - y, x, c, hi], got_y2, here.flip("y")),
            ],
            [
                link.copy(grad.at[k, y, x, c], got_z.at[k - 1], here.shift(k))
                for k in range(first, first + many)
                if k > 0
            ],
        ]

    def step(self, s):
        y, x, c = self.here.y, self.here.x, self.here.c
        g, lo, hi = self.grad, self.lo, self.hi
        got_c, got_y1, got_x2, got_x1, got_y2 = self.got
        if s > 0:
            arrive(self.stages[s - 1])
        if s == 1:
            add_into(g.at[:, :, :, c], got_c, 3)
        if s == 2:
            add_into(g.at[:, y, :, c, lo], got_y1, 2)
            add_into(g.at[:, :, x, c, hi], got_x1, 2)
        if s == 3:
            add_into(g.at[:, y, x, c, lo], got_x2, 1)
            add_into(g.at[:, y, x, c, hi], got_y2, 1)
        if s < 4:
            start(self.stages[s])

    def drain(self):
        for copies in self.stages:
            left(copies)


def normalize(values):
    average = jnp.mean(values, axis=-1, keepdims=True)
    centered = values - average
    spread = jnp.mean(centered * centered, axis=-1, keepdims=True)
    scale = lax.rsqrt(spread + 1e-06)
    return centered * scale, scale


def normalize_back(hat, scale, gain, grad):
    scaled = grad * gain
    return (
        scaled
        - jnp.mean(scaled, axis=-1, keepdims=True)
        - hat * jnp.mean(scaled * hat, axis=-1, keepdims=True)
    ) * scale


def select(values, pick):
    high = values.astype(BF16)
    rest = values - high.astype(F32)
    middle = rest.astype(BF16)
    low = (rest - middle.astype(F32)).astype(BF16)
    return mm(high, pick) + mm(middle, pick) + mm(low, pick)


ROWS = 64
UNITS = 5
NAMES = (
    "tokens",
    "cot",
    "segments",
    "ln1_gain",
    "ln1_bias",
    "out_bias",
    "ln2_gain",
    "ln2_bias",
    "fc2_bias",
    "qv_bias",
    "fc1_bias",
    "w_qkv",
    "w_out",
    "w_fc1",
    "w_fc2",
)
OUTS = (
    "output",
    "g_tokens",
    "s_qkv",
    "s_out",
    "s_fc1",
    "s_fc2",
    "small",
    "cls",
)
SCRATCH = (
    "f_qkv",
    "f_out",
    "f_fc1",
    "f_fc2",
    "biases",
    "normed",
    "mixed",
    "mask",
    "lse",
    "heads",
    "resid",
    "normed2",
    "active",
    "slope",
    "turned",
    "acc",
    "g_low",
    "g_heads",
    "g_fc2",
    "g_out",
    "cols",
    "sums",
    "got_small",
    "all_sums",
)


def layer_kernel(dp_size, parts, heads, *refs):
    refs = list(refs)
    ref = {}
    for name in NAMES + OUTS + SCRATCH:
        ref[name] = refs.pop(0)
    got = [[refs.pop(0) for _ in range(5)] for _ in range(UNITS + parts)]
    got_z = [refs.pop(0) for _ in range(UNITS + 1)]
    local_sem, send_sem, recv_sem = refs
    tokens, cot, cols, vecs = ref["tokens"], ref["cot"], ref["cols"], ref["biases"].at[0]
    segments = ref["segments"]
    f_qkv, f_out, f_fc1, f_fc2 = ref["f_qkv"], ref["f_out"], ref["f_fc1"], ref["f_fc2"]
    biases, normed, mixed, mask = ref["biases"], ref["normed"], ref["mixed"], ref["mask"]
    lse, hd, resid, normed2 = ref["lse"], ref["heads"], ref["resid"], ref["normed2"]
    active, slope, turned, acc = ref["active"], ref["slope"], ref["turned"], ref["acc"]
    tile = acc.at[:, pl.ds(0, 256)]
    g_low, g_heads, sums = ref["g_low"], ref["g_heads"], ref["sums"]
    g_fc2, g_out = ref["g_fc2"], ref["g_out"]
    g_mixed = active
    wide = f_qkv.shape[5]
    g_qkv = f_fc1.at[:, :, :, :, :, pl.ds(0, wide)]
    g_fc1 = f_fc2
    width = tokens.shape[1]
    small = sums.at[0]
    here = Place(dp_size, parts)
    qk_wide = heads * 128
    strides = [1 << b for b in range(dp_size.bit_length() - 1)]
    bits = [here.flip_stride(s) for s in strides]
    link = Link(send_sem, recv_sem)

    shards = [ref[n] for n in ("w_qkv", "w_out", "w_fc1", "w_fc2")]
    wholes = [f_qkv, f_out, f_fc1, f_fc2]
    own = [
        pltpu.make_async_copy(shards[i], wholes[i].at[0], local_sem.at[i]) for i in (0, 2, 3)
    ]
    blocks = shards[1].shape[0]
    places = [f_out.at[0, b // 4, (b // 2) % 2, b % 2] for b in range(FAN)]
    own_out = [
        pltpu.make_async_copy(shards[1].at[b], places[b], local_sem.at[4 + b]) for b in range(blocks)
    ]
    start(own_out + own)
    for b in range(blocks, FAN):
        places[b][...] = jnp.zeros_like(places[b])
    for i, name in enumerate(NAMES[3:11]):
        lanes = ref[name][...].astype(F32)
        for b in range(lanes.shape[0]):
            vecs[i : i + 1, pl.ds(b * 128, 128)] = lanes[b : b + 1]
    greet(bits + [here.shift(k) for k in range(1, parts)])
    def columns(array, first, many):
        return array.at[:, :, :, :, pl.ds(first, many)] if len(array.shape) == 5 else array.at[:, :, :, :, :, pl.ds(first, many)]

    cut = f_fc1.shape[5] // 2
    plans = {"q": gather_unit(here, link, shards[0], f_qkv), "o": gather_unit(here, link, f_out.at[0], f_out)}
    for name, i, first in (("a", 2, 0), ("b", 2, cut), ("c", 3, 0), ("d", 3, cut)):
        plans[name] = gather_unit(
            here, link, columns(shards[i], first, cut), columns(wholes[i], first, cut)
        )
    plans["q"].extra = [
        link.copy(biases.at[0], biases.at[parts - k], here.shift(k)) for k in range(1, parts)
    ]
    for made in own_out:
        made.wait()
    for name in "qoa":
        plans[name].begin()
    units = {}
    for i, (name, grad) in enumerate(
        (
            ("A", columns(g_fc2, 0, cut)),
            ("B", columns(g_fc2, cut, cut)),
            ("C", columns(g_fc1, 0, cut)),
            ("D", columns(g_fc1, cut, cut)),
        )
    ):
        units[name] = Reduction(here, link, grad, 0, parts, got[i], got_z[i])
    units["O"] = Reduction(here, link, g_out, 0, parts, got[UNITS - 1], got_z[UNITS - 1])
    for k in range(parts):
        units[k] = Reduction(here, link, g_qkv, k, 1, got[UNITS + k], got_z[UNITS])

    def fwd(*steps):
        def run():
            for name, s in steps:
                if s == "go":
                    plans[name].begin()
                else:
                    plans[name].step(s)

        return run

    def red(*steps):
        def run():
            for name, s in steps:
                units[name].step(s)

        return run

    def total(grad, got_last, out=None):
        value = grad[0, here.y, here.x, here.c].astype(F32)
        for k in range(parts - 1):
            value += got_last[k].astype(F32)
        if out is None:
            return value
        out[...] = value

    trips = [
        link.copy(sums.at[r], ref["got_small"].at[r], partner) for r, partner in enumerate(bits)
    ]
    all_sums = ref["all_sums"]
    spread_out = [
        link.copy(sums.at[len(bits)], all_sums.at[here.t], here.shift(k)) for k in range(1, parts)
    ]

    def small_round(r):
        if r > 0:
            arrive([trips[r - 1]])
            sums[r] = sums[r - 1] + ref["got_small"][r - 1]
        if r < len(trips):
            start([trips[r]])
        else:
            start(spread_out)
            all_sums[here.t] = sums[r]

    def gain(i):
        return vecs[pl.ds(i, 1), :].astype(F32)

    chunks = SEQ // ROWS

    def rows_of(i):
        return pl.ds(pl.multiple_of(i * ROWS, ROWS), ROWS)

    small[...] = jnp.zeros_like(small)
    labels = jnp.concatenate(
        [segments[pl.ds(here.t * (SEQ // 128) + i, 1), :] for i in range(SEQ // 128)], axis=1
    )
    spot = lax.broadcasted_iota(jnp.int32, (1, SEQ), 1)
    earlier = pltpu.roll(labels, 1, 1)
    begins = (labels >= 0) & ((spot == 0) | (labels != earlier))
    line = labels.astype(F32)
    kinds = lax.broadcasted_iota(jnp.int32, (8, SEQ), 0)
    stacked = jnp.where(kinds == 0, line, jnp.where(kinds == 1, (labels >= 0).astype(F32), begins.astype(F32)))
    cols[...] = stacked.T

    def norm_one(i):
        r = rows_of(i)
        hat, _ = normalize(tokens[r, :].astype(F32))
        normed[r, :] = (hat * gain(0) + gain(1)).astype(BF16)
        mask[r, :] = jnp.where(cols[r, 0:1] == line, 0.0, -1e30)

    loop(chunks, norm_one)
    start(plans["q"].extra)

    low_half = lax.broadcasted_iota(jnp.int32, (SEQ, 128), 1) < 64

    head_cols = heads * HD
    pick = active.at[0, pl.ds(0, 2 * head_cols), pl.ds(0, wide)]
    taken = lax.broadcasted_iota(jnp.int32, (2 * head_cols, wide), 0)
    slot = lax.broadcasted_iota(jnp.int32, (2 * head_cols, wide), 1)
    lane = slot % 128
    of_q = (slot < qk_wide) & (lane < HD) & (taken == (slot // 128) * HD + lane)
    of_v = (slot >= qk_wide) & (taken == head_cols + slot - qk_wide)
    pick[...] = jnp.where(of_q | of_v, 1.0, 0.0).astype(BF16)

    def qkv_part(k):
        offset = mm(biases[k, :, pl.ds(0, 2 * head_cols)].astype(BF16), pick[...])[6:7]
        for at in range(0, wide, 256):
            size = min(256, wide - at)
            w = f_qkv[k, :, :, :, :, pl.ds(at, size)].reshape(width, size)
            out = mm(normed[...], w) + offset[:, at : at + size]
            mixed[k, :, pl.ds(at, size)] = out.astype(BF16)

    def head_place(i):
        k, j = i // heads, i % heads
        at = pl.ds(pl.multiple_of(j * 128, 128), 128)
        v_at = pl.ds(pl.multiple_of(qk_wide + (j // 2) * 128, 128), 128)
        h_at = pl.ds(pl.multiple_of((j // 2) * 128, 128), 128)
        even = j % 2 == 0
        return k, at, v_at, h_at, even

    def scores_of(k, at):
        qk = mixed[k, :, at].astype(F32)
        q = jnp.where(low_half, qk * (1.0 / math.sqrt(HD)), 0.0).astype(BF16)
        kq = pltpu.roll(qk, 64, 1).astype(BF16)
        return mm_nt(kq, q) + mask[...], kq

    def mine_of(even):
        return low_half == even

    def attend(i):
        k, at, v_at, h_at, even = head_place(i)
        scores, _ = scores_of(k, at)
        highest = jnp.max(scores, axis=0, keepdims=True)
        expon = jnp.exp(scores - highest)
        total = jnp.sum(expon, axis=0, keepdims=True)
        lse[i, 0:1, :] = highest + jnp.log(total)
        weights = (expon * (1.0 / total)).astype(BF16)
        out = mm_tn(weights, mixed[k, :, v_at])
        before = jnp.where(even, 0.0, hd[k, :, h_at].astype(F32))
        hd[k, :, h_at] = jnp.where(mine_of(even), out, before).astype(BF16)

    own[0].wait()
    qkv_part(0)
    loop(heads, attend, {1: fwd(("q", "z"))})
    fwd(("o", "z"), ("b", "go"), ("q", 0), ("o", 0))()
    fwd(("a", "z"), ("c", "go"), ("q", 1), ("a", 0), ("o", 1), ("b", "z"), ("d", "go"), ("q", 2))()
    fwd(("b", 0), ("a", 1), ("c", "z"), ("q", 3))()
    loop(parts - 1, lambda k: qkv_part(k + 1))
    loop(
        heads * (parts - 1),
        lambda i: attend(i + heads),
        {
            0: fwd(("o", 2), ("c", 0)),
            1: fwd(("b", 1), ("d", "z")),
            2: fwd(("d", 0)),
            5: fwd(("a", 2), ("o", 3)),
        },
    )
    for made in own[1:]:
        made.wait()

    def project(n):
        at = pl.ds(pl.multiple_of(n * 256, 256), 256)
        total = tokens[:, at].astype(F32) + vecs[2:3, at].astype(F32)
        for k in range(parts):
            total += mm(hd[k], f_out[k, :, :, :, :, at].reshape(-1, 256))
        resid[:, at] = total

    loop(width // 256, project)
    fwd(("b", 2), ("a", 3))()

    def norm_two(i):
        r = rows_of(i)
        hat, _ = normalize(resid[r, :])
        normed2[r, :] = (hat * gain(3) + gain(4)).astype(BF16)

    loop(chunks, norm_two)
    fwd(("c", 1))()
    hid = f_fc1.shape[5]
    tiles = hid // 256

    def fc1_tile(i):
        k, n = i // tiles, i % tiles
        at = pl.ds(pl.multiple_of(n * 256, 256), 256)
        tile[...] = mm(normed2[...], f_fc1[k, :, :, :, :, at].reshape(width, 256)) + biases[
            k, 7:8, at
        ].astype(F32)

        def gelu(j):
            r = rows_of(j)
            v = tile[r, :]
            cdf = 0.5 * (1.0 + lax.erf(v * (1.0 / math.sqrt(2.0))))
            pdf = jnp.exp(-0.5 * v * v) * (1.0 / math.sqrt(2.0 * math.pi))
            active[k, r, at] = (v * cdf).astype(BF16)
            slope[k, r, at] = (cdf + v * pdf).astype(BF16)

        loop(chunks, gelu)

    loop(tiles, fc1_tile)
    fwd(("b", 3), ("d", 1))()
    loop(
        tiles * (parts - 1),
        lambda i: fc1_tile(i + tiles),
        {7: fwd(("c", 2))},
    )

    def grad_branch(i):
        r = rows_of(i)
        g_low[r, :] = (cot[r, :].astype(F32) * cols[r, 1:2]).astype(BF16)

    loop(chunks, grad_branch)
    ones = jnp.ones((8, SEQ), BF16)

    def turn(source):
        def body(n):
            at = pl.ds(pl.multiple_of(n * 256, 256), 256)
            turned[at, :] = source[:, at].astype(F32).T.astype(BF16)

        loop(width // 256, body)

    def weight_grad(target, source, columns, parts_here=parts):
        def body(k):
            for at in range(0, columns, 256):
                size = min(256, columns - at)
                out = mm(turned[...], source[k, :, pl.ds(at, size)])
                target[k, :, :, :, :, pl.ds(at, size)] = out.astype(BF16).reshape(
                    2, 2, 2, width // FAN, size
                )

        return body

    turn(g_low)
    small[1:2, :] = mm(ones, g_low[...])[0:1]
    loop(parts, weight_grad(g_fc2, active, hid))
    red(("A", 0), ("B", 0))()
    fwd(("d", 2), ("c", 3), ("d", 3))()
    for plan in plans.values():
        plan.drain()

    def finish(n):
        at = pl.ds(pl.multiple_of(n * 256, 256), 256)
        total = resid[:, at] + vecs[5:6, at].astype(F32)
        for k in range(parts):
            total += mm(active[k], f_fc2[k, :, :, :, :, at].reshape(hid, 256))
        out = total.astype(BF16)
        ref["output"][:, at] = out
        values = out.astype(F32)
        picked = values * cols[:, 2:3]
        small[4:5, at] = jnp.sum(picked, axis=0, keepdims=True)
        small[5:6, at] = jnp.sum(picked * values, axis=0, keepdims=True)

    loop(width // 256, finish, {1: red(("A", 1)), 2: red(("B", 1))})
    small[6:7, :] = jnp.broadcast_to(jnp.sum(cols[:, 2:3], axis=0, keepdims=True), (1, width))
    side = hid // 2

    def hidden_back(i):
        k, s = i // 2, i % 2
        at = pl.ds(pl.multiple_of(s * side, 128), side)
        back = mm_nt(g_low[...], f_fc2[k, s].reshape(side, width))
        back = (back * slope[k, :, at].astype(F32)).astype(BF16)
        slope[k, :, at] = back
        row = pl.ds(10 + (here.t + k) % parts, 1)
        small[row, at] = mm(ones, back)[0:1]

    loop(2 * parts, hidden_back, {6: red(("A", 2))})
    turn(normed2)
    loop(parts, weight_grad(g_fc1, slope, hid))
    red(("C", 0), ("D", 0), ("B", 2))()

    def normed2_back(s):
        at = pl.ds(pl.multiple_of(s * side, 128), side)
        total = mm_nt(slope[0], f_fc1[0, s].reshape(side, hid))
        for k in range(1, parts):
            total += mm_nt(slope[k], f_fc1[k, s].reshape(side, hid))
        acc[:, at] = total

    loop(2, normed2_back, {1: red(("C", 1))})
    red(("D", 1), ("A", 3))()

    def norm_two_back(i):
        r = rows_of(i)
        grad = acc[r, :]
        hat, scale = normalize(resid[r, :])
        back = cot[r, :].astype(F32) * cols[r, 1:2] + normalize_back(hat, scale, gain(3), grad)
        acc[r, :] = back
        g_low[r, :] = back.astype(BF16)
        small[2:3, :] += jnp.sum(grad * hat, axis=0, keepdims=True)
        small[3:4, :] += jnp.sum(grad, axis=0, keepdims=True)
        small[0:1, :] += jnp.sum(back, axis=0, keepdims=True)

    loop(chunks, norm_two_back)
    turn(g_low)
    v_wide = hd.shape[2]
    loop(parts, weight_grad(g_out, hd, v_wide))
    red(("O", 0), ("B", 3))()

    def heads_back(k):
        g_heads[k] = mm_nt(g_low[...], f_out[k].reshape(v_wide, width)).astype(BF16)

    loop(parts, heads_back)

    def attend_back(i):
        k, at, v_at, h_at, even = head_place(i)
        mine = mine_of(even)
        scores, kq = scores_of(k, at)
        weights = jnp.exp(scores - lse[i, 0:1, :])
        grad = g_heads[k, :, h_at]
        own_grad = jnp.where(mine, grad.astype(F32), 0.0).astype(BF16)
        g_value = mm(weights.astype(BF16), grad)
        g_weights = mm_nt(mixed[k, :, v_at], own_grad)
        inner = jnp.sum(g_weights * weights, axis=0, keepdims=True)
        g_scores = (weights * (g_weights - inner)).astype(BF16)
        g_q = mm_tn(g_scores, kq)
        g_k = mm(g_scores, kq)
        both = jnp.where(low_half, g_q, g_k) * (1.0 / math.sqrt(HD))
        g_mixed[k, :, at] = both.astype(BF16)
        before = jnp.where(even, 0.0, g_mixed[k, :, v_at].astype(F32))
        g_mixed[k, :, v_at] = jnp.where(mine, g_value, before).astype(BF16)

    turn(normed)

    def qkv_grad(k):
        def run():
            weight_grad(g_qkv, g_mixed, wide)(k)
            units[k].step(0)
            row = pl.ds(10 + parts + (here.t + k) % parts, 1)
            small[row, pl.ds(0, wide)] = mm(ones, g_mixed[k, :, pl.ds(0, wide)])[0:1]

        return run

    hooks = {}

    def hook(at, *runs):
        hooks.setdefault(at, []).extend(runs)

    for k in range(1, parts):
        hook(heads * k, qkv_grad(k - 1))
    hook(1, red(("C", 2)))
    hook(2, red(("O", 1)))
    hook(5, red(("D", 2)))
    hook(7, red((0, 1)))
    hook(8, red(("A", 4), ("C", 3)))
    hook(9, red((1, 1)))
    hook(10, red(("O", 2)))
    hook(11, red(("D", 3), (0, 2)))

    def joined(runs):
        def run():
            for one in runs:
                one()

        return run

    loop(heads * parts, attend_back, {at: joined(runs) for at, runs in hooks.items()})
    qkv_grad(parts - 1)()
    for k in range(2, parts - 1):
        red((k, 1))()

    def normed_back(s):
        at = pl.ds(pl.multiple_of(s * side, 128), side)
        total = mm_nt(g_mixed[0, :, pl.ds(0, wide)], f_qkv[0, s].reshape(side, wide))
        for k in range(1, parts):
            total += mm_nt(g_mixed[k, :, pl.ds(0, wide)], f_qkv[k, s].reshape(side, wide))
        tile_out = total
        resid[:, at] = tile_out

    loop(2, normed_back, {1: red((parts - 1, 1), (1, 2), ("O", 3))})

    def norm_one_back(i):
        r = rows_of(i)
        grad = resid[r, :]
        hat, scale = normalize(tokens[r, :].astype(F32))
        back = acc[r, :] + normalize_back(hat, scale, gain(0), grad)
        ref["g_tokens"][r, :] = back.astype(BF16)
        small[8:9, :] += jnp.sum(grad * hat, axis=0, keepdims=True)
        small[9:10, :] += jnp.sum(grad, axis=0, keepdims=True)

    loop(chunks, norm_one_back)
    small_round(0)
    for k in range(2, parts):
        red((k, 2))()
    red(("B", 4), ("C", 4), ("D", 4), ("O", 4))()
    small_round(1)
    total(columns(g_fc1, 0, cut), got_z[2], ref["s_fc1"].at[:, pl.ds(0, cut)])
    total(columns(g_fc1, cut, cut), got_z[3], ref["s_fc1"].at[:, pl.ds(cut, cut)])
    for k in range(parts):
        red((k, 3))()
    small_round(2)
    total(g_out, got_z[UNITS - 1], ref["s_out"])
    for r in range(3, len(trips) + 1):
        small_round(r)
    for i, first in enumerate((0, cut)):
        total(columns(g_fc2, first, cut), got_z[i], ref["s_fc2"].at[:, pl.ds(first, cut)])
    for k in range(parts):
        red((k, 4))()
    triple = 3 * HD
    source = lax.broadcasted_iota(jnp.int32, (wide, heads * triple), 0)
    target = lax.broadcasted_iota(jnp.int32, (wide, heads * triple), 1)
    head, lane = target // triple, target % triple
    wanted = jnp.where(lane < 2 * HD, head * 2 * HD + lane, qk_wide + head * HD + lane - 2 * HD)
    unpick = jnp.where(source == wanted, 1.0, 0.0).astype(BF16)
    ref["s_qkv"][...] = select(total(g_qkv, got_z[UNITS]), unpick)
    arrive(spread_out)
    final = all_sums[0]
    for t in range(1, parts):
        final += all_sums[t]
    ref["small"][...] = final
    source = lax.broadcasted_iota(jnp.int32, (wide, 2 * head_cols), 0)
    target = lax.broadcasted_iota(jnp.int32, (wide, 2 * head_cols), 1)
    wanted = jnp.where(
        target < head_cols, (target // HD) * 2 * HD + target % HD, qk_wide + target - head_cols
    )
    ref["small"][pl.ds(10 + parts, parts), pl.ds(0, 2 * head_cols)] = select(
        final[:, :wide], jnp.where(source == wanted, 1.0, 0.0).astype(BF16)
    )[10 + parts : 10 + 2 * parts]
    mean = final[4:5, :] / final[6:7, :]
    spread = final[5:6, :] / final[6:7, :] - mean * mean
    spread = lax.rsqrt(spread + 1e-05)

    def features(i):
        r = rows_of(i)
        ref["cls"][r, :] = cols[r, 2:3] * (ref["output"][r, :].astype(F32) - mean) * spread

    loop(chunks, features)
    left(trips + spread_out)
    for unit in units.values():
        unit.drain()


def layer(tokens, cot, segments, vectors, shards, dp_size, parts, heads):
    width, hid, wide = tokens.shape[1], shards[2].shape[1], shards[0].shape[1]
    v_wide = -(-heads // 2) * 2 * HD
    piece = v_wide // FAN
    whole = [pltpu.VMEM((parts, 2, 2, 2, rows // FAN, n), BF16) for rows, n in ((width, wide), (v_wide, width), (width, hid), (hid, width))]
    shards = [
        s.reshape(-1, piece, width) if i == 1 else s.reshape(2, 2, 2, s.shape[0] // FAN, s.shape[1])
        for i, s in enumerate(shards)
    ]
    line = max(v.shape[0] for v in vectors)
    lines = -(-(10 + 2 * parts) // 8) * 8
    rounds = dp_size.bit_length() - 1
    copies = 6 * (5 + parts + 1) + parts - 1 + (UNITS + parts) * (5 + parts) + rounds + parts
    blk = width // FAN
    grads = [(blk, wide), (blk, v_wide), (blk, hid), (blk, hid)]
    scratch = whole + [
        pltpu.VMEM((parts, len(vectors), line), F32),
        pltpu.VMEM((SEQ, width), BF16),
        pltpu.VMEM((parts, SEQ, wide), BF16),
        pltpu.VMEM((SEQ, SEQ), F32),
        pltpu.VMEM((parts * heads, 8, SEQ), F32),
        pltpu.VMEM((parts, SEQ, v_wide), BF16),
        pltpu.VMEM((SEQ, width), F32),
        pltpu.VMEM((SEQ, width), BF16),
        pltpu.VMEM((parts, SEQ, hid), BF16),
        pltpu.VMEM((parts, SEQ, hid), BF16),
        pltpu.VMEM((width, SEQ), BF16),
        pltpu.VMEM((SEQ, width), F32),
        pltpu.VMEM((SEQ, width), BF16),
        pltpu.VMEM((parts, SEQ, v_wide), BF16),
        pltpu.VMEM((parts, 2, 2, 2, blk, hid), BF16),
        pltpu.VMEM((parts, 2, 2, 2, blk, v_wide), BF16),
        pltpu.VMEM((SEQ, 8), F32),
        pltpu.VMEM((rounds + 1, lines, width), F32),
        pltpu.VMEM((rounds, lines, width), F32),
        pltpu.VMEM((parts, lines, width), F32),
    ]
    sizes = [(parts, hid // 2)] * 4 + [(parts, v_wide)] + [(1, wide)] * parts
    for many, n in sizes:
        for lead, half in (((many, 2, 2), 1), ((many, 2), 2), ((many,), 2), ((many, 2), 2), ((many,), 2)):
            scratch.append(pltpu.VMEM(lead + (blk // half, n), BF16))
    for _, n in sizes[: UNITS + 1]:
        scratch.append(pltpu.VMEM((parts - 1, blk, n), BF16))
    scratch += [
        pltpu.SemaphoreType.DMA((4 + FAN,)),
        pltpu.SemaphoreType.DMA((copies,)),
        pltpu.SemaphoreType.DMA((copies,)),
    ]
    shape = jax.ShapeDtypeStruct
    return pl.pallas_call(
        partial(layer_kernel, dp_size, parts, heads),
        out_shape=[shape(tokens.shape, BF16), shape(tokens.shape, BF16)]
        + [shape((blk, heads * 3 * HD), F32), shape((blk, v_wide), F32), shape((blk, hid), F32), shape((blk, hid), F32)]
        + [shape((lines, width), F32), shape(tokens.shape, F32)],
        in_specs=[VMEM] * (3 + len(vectors)) + [ANY] * 4,
        out_specs=[VMEM] * 8,
        scratch_shapes=scratch,
        compiler_params=pltpu.CompilerParams(
            collective_id=0, has_side_effects=True, vmem_limit_bytes=67043328
        ),
    )(tokens, cot, segments, *[v.reshape(-1, 128) for v in vectors], *shards)


def regroup(columns, heads):
    wide = heads * 2 * HD + -(-heads // 2) * 2 * HD
    wanted = np.arange(heads * 3 * HD).reshape(heads, 3, HD)
    source = np.concatenate([wanted[:, :2].reshape(-1), wanted[:, 2].reshape(-1)])
    pick = np.zeros((heads * 3 * HD, wide), np.float32)
    pick[source, np.arange(source.size)] = 1.0
    return jnp.dot(columns, jnp.asarray(pick, BF16), preferred_element_type=F32).astype(BF16)


def on_device(dp_size, parts, tokens, segments, cotangent, ln1_gain, ln1_bias, w_qkv, q_bias, v_bias, w_out, out_bias, ln2_gain, ln2_bias, w_fc1, fc1_bias, w_fc2, fc2_bias):
    tensor_index = lax.axis_index("tensor")
    rows, width = tokens.shape
    head_cols = w_out.shape[0]
    heads = head_cols // HD
    hidden_cols = w_fc1.shape[1]
    qkv = regroup(w_qkv, heads)
    vectors = [ln1_gain, ln1_bias, out_bias, ln2_gain, ln2_bias, fc2_bias, jnp.concatenate([q_bias, v_bias]), fc1_bias]

    output, grad_tokens, sum_qkv, sum_out, sum_fc1, sum_fc2, small, cls_features = layer(
        tokens, cotangent, segments.reshape(-1, 128), vectors, [qkv, w_out, w_fc1, w_fc2], dp_size, parts, heads
    )
    low = dp_size // FAN

    def finish(array, axis):
        if low == 1:
            return array
        groups = [[i * low + j for j in range(low)] for i in range(FAN)]
        return lax.psum_scatter(array, "dp", scatter_dimension=axis, axis_index_groups=groups, tiled=True)

    sum_qkv, sum_fc1, sum_out, sum_fc2 = (
        finish(a, 0) for a in (sum_qkv, sum_fc1, sum_out[:, :head_cols], sum_fc2)
    )
    start = 10 + parts
    mixed_sums = small[start : start + parts]
    return (
        output,
        grad_tokens,
        cls_features,
        sum_qkv,
        mixed_sums[:, :head_cols].reshape(-1),
        mixed_sums[:, head_cols : 2 * head_cols].reshape(-1),
        sum_out.T,
        small[0],
        sum_fc1,
        small[10 : 10 + parts, :hidden_cols].reshape(-1),
        sum_fc2.T,
        small[1],
        small[8],
        small[9],
        small[2],
        small[3],
    )


def solution(mesh):
    dp_size, parts = mesh.shape["dp"], mesh.shape["tensor"]
    row, whole, cols, out_cols = P(("dp", "tensor"), None), P(), P(None, "tensor"), P("tensor")
    down = P("tensor", None)
    in_specs = (row, P("dp"), row, whole, whole, cols, out_cols, out_cols, down, whole, whole, whole, cols, out_cols, down, whole)
    spread, turned = P("dp", "tensor"), P("tensor", "dp")
    out_specs = (row, row, row, spread, whole, whole, turned, whole, spread, whole, turned, whole, whole, whole, whole, whole)
    return jax.shard_map(partial(on_device, dp_size, parts), mesh=mesh, in_specs=in_specs, out_specs=out_specs, check_vma=False)
```
